128 devices in a mesh: gx: 8 (over z, core), gy: 8 (over y, x_lo), gz: 2 (over x_hi).
Axes of the slice: x: 4 (x_hi: 2, x_lo: 2; x = x_hi * 2 + x_lo), y: 4, z: 4, core: 2. Of those that a mesh axis runs over, the one named last changes fastest.
Arguments:
- grads: float32 [8, 8, 2, 16, 14336], P('gx', 'gy', 'gz'), may hold values from -100 to 100
- plan: int32 [3], replicated, may hold values from 0 to 2, each once
Outputs:
- averaged: float32 [8, 8, 2, 16, 14336], P('gx', 'gy', 'gz')
- reports: float32 [3], replicated
The draws below stay inside these ranges and needn't reach their ends.
Inputs may be any that keep to these rules, and one draw needn't show every extreme that they name: `plan`: each of 0, 1, 2 appears once.
All inputs are finite; a program needn't handle non-finite values.
Results may differ from the reference program's by a relative error of at most 0.0003.
Values sent between devices are 32-bit elements; how exact they have to be, the bound alone decides.
No kernel may reach another device: no remote copies, remote signals or barrier semaphores. Data moves between devices by JAX's collectives and lax.ppermute only.
A program may use at most 64 MiB of HBM per device.

```python
import math
import jax
import jax.numpy as jnp
from jax import lax

FF = 14336
ROWS = 16
N_GX = 8
N_GY = 8
N_GZ = 2


def draw_grads(key, part):
    first, second = jax.random.split(jax.random.fold_in(key, 17), 2)
    scales = jnp.exp(jax.random.uniform(first, (N_GX, N_GY, N_GZ, 1, 1), jnp.float32) * math.log(3.0))
    base = jax.random.normal(second, (N_GX, N_GY, N_GZ, ROWS, FF), jnp.float32)
    base = jnp.clip(base, -6.0, 6.0)
    return (base * scales).astype(jnp.float32)


def setup_inputs(seed: int = 0) -> dict:
    key_of = jax.random.split(jax.random.key(seed), 3)
    return {
        "grads": draw_grads(jax.random.fold_in(key_of[2], 71), 0),
        "plan": jax.random.permutation(key_of[1], 3).astype(jnp.int32),
    }


def one_round(current, axis_id):
    def along(dim):
        def inner(value):
            total = jnp.sum(value, axis=dim, keepdims=True)
            return jnp.broadcast_to(total / value.shape[dim], value.shape)
        return inner
    group = lax.switch(axis_id, [along(0), along(1), along(2)], current)
    deviation = jnp.max(jnp.abs(current - group))
    return group, deviation


def reference(grads, plan):
    current = grads
    values = []
    for step in range(3):
        current, deviation = one_round(current, plan[step])
        values.append(deviation)
    return current, jnp.stack(values).astype(jnp.float32)
```

```python
import jax
import jax.numpy as jnp
from jax import lax
from jax.experimental import pallas as pl
from jax.experimental.pallas import tpu as pltpu
from jax.sharding import Mesh
from jax.sharding import PartitionSpec as P

PLANE = ("z", "y", "x_lo", "x_hi")
EVERY = ("core", *PLANE)
COLS = 128
DATA = 14
CARRIED = 16
ROOM = pltpu.CompilerParams(vmem_limit_bytes=8 * 2**20)


def swap_pairs(rows, apart):
    n = rows.shape[0]
    place = lax.broadcasted_iota(jnp.int32, rows.shape, 0)
    first = (place // apart) % 2 == 0
    return jnp.where(
        first, pltpu.roll(rows, n - apart, 0), pltpu.roll(rows, apart, 0)
    )


def far(worst, value, mean):
    gap = jnp.abs(value - mean)
    return jnp.maximum(worst, jnp.max(gap.reshape(-1, 8, COLS), axis=0))


def rounds(plan_ref, g_ref, share_ref):
    zero = jnp.zeros((8, COLS), jnp.float32)
    mx = []
    for y in range(4):
        total = g_ref[y]
        for gx in range(1, 8):
            total = total + g_ref[gx * 4 + y]
        mx.append(total * 0.125)
    mxz = [(m + swap_pairs(m, DATA)) * 0.5 for m in mx]
    sum_xy = mx[0] + mx[1] + mx[2] + mx[3]
    mxy = (sum_xy + pltpu.roll(sum_xy, 2 * DATA, 0)) * 0.125
    mall = (mxy + swap_pairs(mxy, DATA)) * 0.5

    x = y_ = z = z_xz = z_yz = y_xy = y_yz = yz_all = zero
    for gx in range(8):
        part = [g_ref[gx * 4 + y] for y in range(4)]
        total = (part[0] + part[1]) + (part[2] + part[3])
        my = (total + pltpu.roll(total, 2 * DATA, 0)) * 0.125
        myz = (my + swap_pairs(my, DATA)) * 0.5
        y_xy = far(y_xy, my, mxy)
        y_yz = far(y_yz, my, myz)
        yz_all = far(yz_all, myz, mall)
        for y in range(4):
            mz = (part[y] + swap_pairs(part[y], DATA)) * 0.5
            x = far(x, part[y], mx[y])
            y_ = far(y_, part[y], my)
            z = far(z, part[y], mz)
            z_xz = far(z_xz, mz, mxz[y])
            z_yz = far(z_yz, mz, myz)
    x_xy = x_xz = xz_all = zero
    for y in range(4):
        x_xy = far(x_xy, mx[y], mxy)
        x_xz = far(x_xz, mx[y], mxz[y])
        xz_all = far(xz_all, mxz[y], mall)
    xy_all = far(zero, mxy, mall)

    a, b, c = plan_ref[0], plan_ref[1], plan_ref[2]

    def pick(which, of_x, of_y, of_z):
        return jnp.where(which == 0, of_x, jnp.where(which == 1, of_y, of_z))

    first = pick(a, x, y_, z)
    second = pick(
        a,
        jnp.where(b == 1, x_xy, x_xz),
        jnp.where(b == 0, y_xy, y_yz),
        jnp.where(b == 0, z_xz, z_yz),
    )
    third = pick(c, yz_all, xz_all, xy_all)
    lane = lax.broadcasted_iota(jnp.int32, (2, COLS), 1)
    told = jnp.where(
        lane == 0,
        jnp.max(first),
        jnp.where(lane == 1, jnp.max(second), jnp.max(third)),
    )
    share = jnp.concatenate([mall[:DATA], told], axis=0)
    for i in range(share_ref.shape[0]):
        share_ref[i] = share


def spread(own_ref, other_ref, out_ref, reports_ref, sems):
    core = lax.axis_index("core")
    count = own_ref.shape[0]
    copies = []
    for i, (half, side) in enumerate(((own_ref, core), (other_ref, 1 - core))):
        place = out_ref.at[pl.ds(side * count, count)]
        copies.append(
            pltpu.make_async_copy(half.at[:, : DATA // 2], place, sems.at[i])
        )
        copies[-1].start()
    worst = jnp.maximum(
        jnp.max(own_ref[:, DATA // 2], axis=0),
        jnp.max(other_ref[:, DATA // 2], axis=0),
    )
    lane = lax.broadcasted_iota(jnp.int32, worst.shape, 1)
    for r in range(3):
        reports_ref[r] = jnp.max(jnp.where(lane == r, worst, 0.0))
    for copy in copies:
        copy.wait()


def on_device(grads, plan):
    rows, width = grads.shape[-2:]
    tiles = width // COLS
    count = lax.axis_size(EVERY)
    entries = grads.reshape(rows // 8, 8, tiles, COLS).transpose(0, 2, 1, 3)
    entries = entries.reshape(count, DATA // 2, 2, COLS)
    arrived = lax.all_to_all(entries, EVERY, 0, 0, tiled=True)
    peers = lax.axis_size(PLANE)
    share = pl.pallas_call(
        rounds,
        out_shape=jax.ShapeDtypeStruct((peers, CARRIED, COLS), jnp.float32),
        in_specs=[
            pl.BlockSpec(memory_space=pltpu.SMEM),
            pl.BlockSpec(memory_space=pltpu.VMEM),
        ],
        out_specs=pl.BlockSpec(memory_space=pltpu.VMEM),
        compiler_params=ROOM,
    )(plan, arrived.reshape(count // 4, 4 * DATA, COLS))
    half = lax.all_to_all(share, PLANE, 0, 0, tiled=True)
    half = half.reshape(peers, CARRIED // 2, 2, COLS)
    other = lax.ppermute(half, "core", [(0, 1), (1, 0)])
    whole, reports = pl.pallas_call(
        spread,
        out_shape=(
            jax.ShapeDtypeStruct((count, DATA // 2, 2, COLS), jnp.float32),
            jax.ShapeDtypeStruct((3,), jnp.float32),
        ),
        in_specs=[pl.BlockSpec(memory_space=pltpu.VMEM)] * 2,
        out_specs=(
            pl.BlockSpec(memory_space=pl.ANY),
            pl.BlockSpec(memory_space=pltpu.SMEM),
        ),
        scratch_shapes=[pltpu.SemaphoreType.DMA((2,))],
        compiler_params=ROOM,
    )(half, other)
    whole = whole.reshape(rows // 8, tiles, 8, COLS).transpose(0, 2, 1, 3)
    return whole.reshape(grads.shape), reports


def solution(mesh):
    torus = Mesh(
        mesh.devices.reshape(4, 2, 4, 2, mesh.shape["gz"]),
        ("z", "core", "y", "x_lo", "x_hi"),
    )
    placed = P(("z", "core"), ("y", "x_lo"), "x_hi", None, None)
    return jax.shard_map(
        on_device,
        mesh=torus,
        in_specs=(placed, P()),
        out_specs=(placed, P()),
        check_vma=False,
    )
```

```python
import jax
import jax.numpy as jnp
from jax import lax
from jax.experimental import pallas as pl
from jax.experimental.pallas import tpu as pltpu
from jax.sharding import Mesh
from jax.sharding import PartitionSpec as P

PLANE = ("y", "z", "x_hi", "x_lo")
EVERY = ("core", *PLANE)
COLS = 128
DATA = 14
CARRIED = 16
TILES = 4 * DATA // 8
UPPER = 4
SLOT = COLS // 8
ROOM = pltpu.CompilerParams(vmem_limit_bytes=8 * 2**20)


def both_ways(high, low, mean):
    return jnp.maximum(high - mean, mean - low)


def stats(values):
    total = high = low = values[0]
    for value in values[1:]:
        total = total + value
        high = jnp.maximum(high, value)
        low = jnp.minimum(low, value)
    return total, high, low


def rows_of(tiles):
    return jnp.concatenate(tiles, axis=0)


def tiles_of(rows):
    return [rows[8 * t : 8 * t + 8] for t in range(rows.shape[0] // 8)]


def across_x_hi(tiles):
    turned = {t: pltpu.roll(tiles[t], 4, 0) for t in (0, 3, 4, 5, 6)}
    first = lax.broadcasted_iota(jnp.int32, (8, COLS), 0) < 4
    return [
        jnp.where(first, turned[t + 3], turned[(t + 4) % TILES])
        for t in range(UPPER)
    ]


def across_x_lo(tiles):
    rows = rows_of(tiles)
    n = rows.shape[0]
    place = lax.broadcasted_iota(jnp.int32, rows.shape, 0)
    first = ((place >= 0) & (place < DATA)) | (
        (place >= 2 * DATA) & (place < 3 * DATA)
    )
    return tiles_of(
        jnp.where(
            first, pltpu.roll(rows, n - DATA, 0), pltpu.roll(rows, DATA, 0)
        )
    )


def most(values):
    worst = values[0]
    for value in values[1:]:
        worst = jnp.maximum(worst, value)
    return worst


def gaps(tiles, means):
    return [jnp.abs(t - m) for t, m in zip(tiles, means)]


def packed(eight):
    worst = rows_of([jnp.max(v, axis=0, keepdims=True) for v in eight])
    for apart in (64, 32, 16):
        worst = jnp.maximum(worst, pltpu.roll(worst, apart, 1))
    row = lax.broadcasted_iota(jnp.int32, worst.shape, 0)
    lane = lax.broadcasted_iota(jnp.int32, worst.shape, 1)
    return jnp.max(
        jnp.where(row == lane // SLOT, worst, 0.0), axis=0, keepdims=True
    )


def rounds(g_ref, share_ref):
    where = {
        (gx, y): (gx // 4) * 16 + y * 4 + gx % 4
        for gx in range(8)
        for y in range(4)
    }
    half = lambda tiles: [t * 0.5 for t in tiles]
    mx, dev_x = [None] * 4, []
    my_sum, y_high, y_low = [[] for _ in range(8)], [], []
    load = lambda gx, y, t: g_ref[where[gx, y], 8 * t : 8 * t + 8]

    dev_z = []
    mz_of_y = [[[] for _ in range(UPPER)] for _ in range(4)]
    mz_of_gx = [[[] for _ in range(UPPER)] for _ in range(8)]
    for y in range(4):
        x_stats = []
        for t in range(TILES):
            x_stats.append(stats([load(gx, y, t) for gx in range(8)]))
        mx[y] = [s[0] * 0.125 for s in x_stats]
        dev_x += [both_ways(s[1], s[2], m) for s, m in zip(x_stats, mx[y])]
        for gx in range(8):
            tiles = [load(gx, y, t) for t in range(TILES)]
            for t, other in enumerate(across_x_hi(tiles)):
                mean = (tiles[t] + other) * 0.5
                dev_z.append(jnp.abs(tiles[t] - mean))
                mz_of_y[y][t].append(mean)
                mz_of_gx[gx][t].append(mean)
        dev_x, dev_z = [most(dev_x)], [most(dev_z)]

    my, dev_y = [], []
    for gx in range(8):
        y_stats = [
            stats([load(gx, y, t) for y in range(4)]) for t in range(TILES)
        ]
        total = [s[0] for s in y_stats]
        my.append([(a + b) * 0.125 for a, b in zip(total, across_x_lo(total))])
        dev_y += [both_ways(s[1], s[2], m) for s, m in zip(y_stats, my[gx])]
        dev_y = [most(dev_y)]

    def with_other(tiles):
        return [(a + b) * 0.5 for a, b in zip(tiles, across_x_hi(tiles))]

    mxz = [with_other(m) for m in mx]
    myz = [with_other(m) for m in my]
    mxy = [stats([my[gx][t] for gx in range(8)])[0] * 0.125 for t in range(TILES)]
    mall = with_other(mxy)

    x_xy = most([most(gaps(mx[y], mxy)) for y in range(4)])
    x_xz = most([most(gaps(mx[y][:UPPER], mxz[y])) for y in range(4)])
    y_xy = most([most(gaps(my[gx], mxy)) for gx in range(8)])
    y_yz = most([most(gaps(my[gx][:UPPER], myz[gx])) for gx in range(8)])

    def spread_of(values, means):
        worst = []
        for t in range(UPPER):
            _, high, low = stats(values[t])
            worst.append(both_ways(high, low, means[t]))
        return most(worst)

    z_xz = most([spread_of(mz_of_y[y], mxz[y]) for y in range(4)])
    z_yz = most([spread_of(mz_of_gx[gx], myz[gx]) for gx in range(8)])
    xy_all = most(gaps(mxy[:UPPER], mall))
    xz_all = most([most(gaps(mxz[y], mall)) for y in range(4)])
    yz_all = most([most(gaps(myz[gx], mall)) for gx in range(8)])

    none = jnp.zeros((8, COLS), jnp.float32)
    slots = [dev_x[0], dev_y[0], dev_z[0]]
    slots += [none, x_xy, x_xz, y_xy, none, y_yz, z_xz, z_yz, none]
    slots += [yz_all, xz_all, xy_all, none]
    told = rows_of([packed(slots[:8]), packed(slots[8:])])
    share = jnp.concatenate([rows_of(mall[:2])[:DATA], told], axis=0)
    for i in range(share_ref.shape[0]):
        share_ref[i] = share


def place(half_ref, out_ref, side, sem):
    count = half_ref.shape[0]
    return pltpu.make_async_copy(
        half_ref.at[:, : DATA // 2],
        out_ref.at[pl.ds(side * count, count)],
        sem,
    )


def put_own(own_ref, out_ref, sem):
    copy = place(own_ref, out_ref, lax.axis_index("core"), sem)
    copy.start()
    copy.wait()


def put_other(
    plan_ref, own_ref, other_ref, _, out_ref, reports_ref, plan_here, sems
):
    asked = pltpu.make_async_copy(plan_ref, plan_here, sems.at[1])
    asked.start()
    copy = place(other_ref, out_ref, 1 - lax.axis_index("core"), sems.at[0])
    copy.start()
    worst = jnp.maximum(
        jnp.max(own_ref[:, DATA // 2], axis=0),
        jnp.max(other_ref[:, DATA // 2], axis=0),
    )
    row = lax.broadcasted_iota(jnp.int32, worst.shape, 0)
    lane = lax.broadcasted_iota(jnp.int32, worst.shape, 1)
    slot = 8 * row + lane // SLOT
    asked.wait()
    a, b, c = plan_here[0], plan_here[1], plan_here[2]
    for r, wanted in enumerate((a, 3 + 3 * a + b, 12 + c)):
        reports_ref[r] = jnp.max(jnp.where(slot == wanted, worst, 0.0))
    copy.wait()


def on_device(grads, plan):
    rows, width = grads.shape[-2:]
    tiles = width // COLS
    count = lax.axis_size(EVERY)
    vmem = pl.BlockSpec(memory_space=pltpu.VMEM)
    smem = pl.BlockSpec(memory_space=pltpu.SMEM)
    hbm = pl.BlockSpec(memory_space=pl.ANY)
    entries = grads.reshape(rows // 8, 8, tiles, COLS).transpose(0, 2, 1, 3)
    entries = entries.reshape(count, DATA // 2, 2, COLS)
    arrived = lax.all_to_all(entries, EVERY, 0, 0, tiled=True)
    peers = lax.axis_size(PLANE)
    share = pl.pallas_call(
        rounds,
        out_shape=jax.ShapeDtypeStruct((peers, CARRIED, COLS), jnp.float32),
        in_specs=[vmem],
        out_specs=vmem,
        compiler_params=ROOM,
    )(arrived.reshape(count // 4, 4 * DATA, COLS))
    own = lax.all_to_all(share, PLANE, 0, 0, tiled=True)
    own = own.reshape(peers, CARRIED // 2, 2, COLS)
    other = lax.ppermute(own, "core", [(0, 1), (1, 0)])
    whole_type = jax.ShapeDtypeStruct((count, DATA // 2, 2, COLS), jnp.float32)
    cost = pl.CostEstimate(
        flops=10**7, bytes_accessed=own.size * 4, transcendentals=0
    )
    begun = pl.pallas_call(
        put_own,
        out_shape=whole_type,
        in_specs=[vmem],
        out_specs=hbm,
        scratch_shapes=[pltpu.SemaphoreType.DMA],
        compiler_params=ROOM,
        cost_estimate=cost,
    )(own)
    whole, reports = pl.pallas_call(
        put_other,
        out_shape=(whole_type, jax.ShapeDtypeStruct((3,), jnp.float32)),
        in_specs=[hbm, vmem, vmem, hbm],
        out_specs=(hbm, smem),
        scratch_shapes=[
            pltpu.SMEM(plan.shape, plan.dtype),
            pltpu.SemaphoreType.DMA((2,)),
        ],
        input_output_aliases={3: 0},
        compiler_params=ROOM,
    )(plan, own, other, begun)
    whole = whole.reshape(rows // 8, tiles, 8, COLS).transpose(0, 2, 1, 3)
    return whole.reshape(grads.shape), reports


def solution(mesh):
    torus = Mesh(
        mesh.devices.reshape(4, 2, 4, 2, mesh.shape["gz"]),
        ("z", "core", "y", "x_lo", "x_hi"),
    )
    placed = P(("z", "core"), ("y", "x_lo"), "x_hi", None, None)
    return jax.shard_map(
        on_device,
        mesh=torus,
        in_specs=(placed, P()),
        out_specs=(placed, P()),
        check_vma=False,
    )
```

```python
import functools

import jax
import jax.numpy as jnp
from jax import lax
from jax.experimental import pallas as pl
from jax.experimental.pallas import tpu as pltpu
from jax.sharding import Mesh
from jax.sharding import PartitionSpec as P

PLANE = ("y", "z", "x_hi", "x_lo")
EVERY = ("core", *PLANE)
COLS = 128
DATA = 14
CARRIED = 16
TILES = 4 * DATA // 8
UPPER = 4
SLOT = COLS // 8
ROOM = pltpu.CompilerParams(vmem_limit_bytes=8 * 2**20)


def both_ways(high, low, mean):
    return jnp.maximum(high - mean, mean - low)


def stats(values):
    total = high = low = values[0]
    for value in values[1:]:
        total = total + value
        high = jnp.maximum(high, value)
        low = jnp.minimum(low, value)
    return total, high, low


def rows_of(tiles):
    return jnp.concatenate(tiles, axis=0)


def tiles_of(rows):
    return [rows[8 * t : 8 * t + 8] for t in range(rows.shape[0] // 8)]


def across_x_hi(tiles):
    turned = {t: pltpu.roll(tiles[t], 4, 0) for t in (0, 3, 4, 5, 6)}
    first = lax.broadcasted_iota(jnp.int32, (8, COLS), 0) < 4
    return [
        jnp.where(first, turned[t + 3], turned[(t + 4) % TILES])
        for t in range(UPPER)
    ]


def across_x_lo(tiles):
    rows = rows_of(tiles)
    n = rows.shape[0]
    place = lax.broadcasted_iota(jnp.int32, rows.shape, 0)
    first = ((place >= 0) & (place < DATA)) | (
        (place >= 2 * DATA) & (place < 3 * DATA)
    )
    return tiles_of(
        jnp.where(
            first, pltpu.roll(rows, n - DATA, 0), pltpu.roll(rows, DATA, 0)
        )
    )


def most(values):
    worst = values[0]
    for value in values[1:]:
        worst = jnp.maximum(worst, value)
    return worst


def gaps(tiles, means):
    return [jnp.abs(t - m) for t, m in zip(tiles, means)]


def packed(eight):
    worst = rows_of([jnp.max(v, axis=0, keepdims=True) for v in eight])
    for apart in (64, 32, 16):
        worst = jnp.maximum(worst, pltpu.roll(worst, apart, 1))
    row = lax.broadcasted_iota(jnp.int32, worst.shape, 0)
    lane = lax.broadcasted_iota(jnp.int32, worst.shape, 1)
    return jnp.max(
        jnp.where(row == lane // SLOT, worst, 0.0), axis=0, keepdims=True
    )


def rounds(g_ref, share_ref):
    where = {
        (gx, y): (gx // 4) * 16 + y * 4 + gx % 4
        for gx in range(8)
        for y in range(4)
    }
    half = lambda tiles: [t * 0.5 for t in tiles]
    mx, dev_x = [None] * 4, []
    my_sum, y_high, y_low = [[] for _ in range(8)], [], []
    load = lambda gx, y, t: g_ref[where[gx, y], 8 * t : 8 * t + 8]

    dev_z = []
    mz_of_y = [[[] for _ in range(UPPER)] for _ in range(4)]
    mz_of_gx = [[[] for _ in range(UPPER)] for _ in range(8)]
    for y in range(4):
        x_stats = []
        for t in range(TILES):
            x_stats.append(stats([load(gx, y, t) for gx in range(8)]))
        mx[y] = [s[0] * 0.125 for s in x_stats]
        dev_x += [both_ways(s[1], s[2], m) for s, m in zip(x_stats, mx[y])]
        for gx in range(8):
            tiles = [load(gx, y, t) for t in range(TILES)]
            for t, other in enumerate(across_x_hi(tiles)):
                mean = (tiles[t] + other) * 0.5
                dev_z.append(jnp.abs(tiles[t] - mean))
                mz_of_y[y][t].append(mean)
                mz_of_gx[gx][t].append(mean)
        dev_x, dev_z = [most(dev_x)], [most(dev_z)]

    my, dev_y = [], []
    for gx in range(8):
        y_stats = [
            stats([load(gx, y, t) for y in range(4)]) for t in range(TILES)
        ]
        total = [s[0] for s in y_stats]
        my.append([(a + b) * 0.125 for a, b in zip(total, across_x_lo(total))])
        dev_y += [both_ways(s[1], s[2], m) for s, m in zip(y_stats, my[gx])]
        dev_y = [most(dev_y)]

    def with_other(tiles):
        return [(a + b) * 0.5 for a, b in zip(tiles, across_x_hi(tiles))]

    mxz = [with_other(m) for m in mx]
    myz = [with_other(m) for m in my]
    mxy = [stats([my[gx][t] for gx in range(8)])[0] * 0.125 for t in range(TILES)]
    mall = with_other(mxy)

    x_xy = most([most(gaps(mx[y], mxy)) for y in range(4)])
    x_xz = most([most(gaps(mx[y][:UPPER], mxz[y])) for y in range(4)])
    y_xy = most([most(gaps(my[gx], mxy)) for gx in range(8)])
    y_yz = most([most(gaps(my[gx][:UPPER], myz[gx])) for gx in range(8)])

    def spread_of(values, means):
        worst = []
        for t in range(UPPER):
            _, high, low = stats(values[t])
            worst.append(both_ways(high, low, means[t]))
        return most(worst)

    z_xz = most([spread_of(mz_of_y[y], mxz[y]) for y in range(4)])
    z_yz = most([spread_of(mz_of_gx[gx], myz[gx]) for gx in range(8)])
    xy_all = most(gaps(mxy[:UPPER], mall))
    xz_all = most([most(gaps(mxz[y], mall)) for y in range(4)])
    yz_all = most([most(gaps(myz[gx], mall)) for gx in range(8)])

    none = jnp.zeros((8, COLS), jnp.float32)
    slots = [dev_x[0], dev_y[0], dev_z[0]]
    slots += [none, x_xy, x_xz, y_xy, none, y_yz, z_xz, z_yz, none]
    slots += [yz_all, xz_all, xy_all, none]
    told = rows_of([packed(slots[:8]), packed(slots[8:])])
    share = jnp.concatenate([rows_of(mall[:2])[:DATA], told], axis=0)
    for i in range(share_ref.shape[0]):
        share_ref[i] = share


def begin(half_ref, out_ref, side, sems):
    count = half_ref.shape[0]
    part = count // sems.shape[0]
    copies = [
        pltpu.make_async_copy(
            half_ref.at[pl.ds(i * part, part), : DATA // 2],
            out_ref.at[pl.ds(side * count + i * part, part)],
            sems.at[i],
        )
        for i in range(sems.shape[0])
    ]
    for copy in copies:
        copy.start()
    return copies


def put_own(
    plan_ref, own_ref, out_ref, worst_ref, asked_ref, plan_here, sems, plan_sem
):
    asked = pltpu.make_async_copy(plan_ref, plan_here, plan_sem)
    asked.start()
    copies = begin(own_ref, out_ref, lax.axis_index("core"), sems)
    worst = jnp.max(own_ref[:, DATA // 2], axis=0)
    worst_ref[...] = worst
    row = lax.broadcasted_iota(jnp.int32, worst.shape, 0)
    lane = lax.broadcasted_iota(jnp.int32, worst.shape, 1)
    slot = 8 * row + lane // SLOT
    asked.wait()
    a, b, c = plan_here[0], plan_here[1], plan_here[2]
    for r, wanted in enumerate((a, 3 + 3 * a + b, 12 + c)):
        asked_ref[r] = jnp.where(slot == wanted, 1.0, 0.0)
    for copy in copies:
        copy.wait()


def put_other(
    worst_ref, asked_ref, other_ref, _, out_ref, reports_ref,
    reports_here, sems, reports_sem,
):
    copies = begin(other_ref, out_ref, 1 - lax.axis_index("core"), sems)
    worst = jnp.maximum(
        worst_ref[...], jnp.max(other_ref[:, DATA // 2], axis=0)
    )
    for r in range(3):
        wanted = asked_ref[r] > 0.0
        reports_here[r] = jnp.max(jnp.where(wanted, worst, 0.0))
    told = pltpu.make_async_copy(reports_here, reports_ref, reports_sem)
    told.start()
    for copy in (*copies, told):
        copy.wait()


def on_device(grads, plan):
    rows, width = grads.shape[-2:]
    tiles = width // COLS
    count = lax.axis_size(EVERY)
    vmem = pl.BlockSpec(memory_space=pltpu.VMEM)
    hbm = pl.BlockSpec(memory_space=pl.ANY)
    entries = grads.reshape(rows // 8, 8, tiles, COLS).transpose(0, 2, 1, 3)
    entries = entries.reshape(count, DATA // 2, 2, COLS)
    arrived = lax.all_to_all(entries, EVERY, 0, 0, tiled=True)
    peers = lax.axis_size(PLANE)
    share = pl.pallas_call(
        rounds,
        out_shape=jax.ShapeDtypeStruct((peers, CARRIED, COLS), jnp.float32),
        in_specs=[vmem],
        out_specs=vmem,
        compiler_params=ROOM,
    )(arrived.reshape(count // 4, 4 * DATA, COLS))
    own = lax.all_to_all(share, PLANE, 0, 0, tiled=True)
    own = own.reshape(peers, CARRIED // 2, 2, COLS)
    other = lax.ppermute(own, "core", [(0, 1), (1, 0)])
    whole_type = jax.ShapeDtypeStruct((count, DATA // 2, 2, COLS), jnp.float32)
    cost = pl.CostEstimate(
        flops=10**7, bytes_accessed=own.size * 4, transcendentals=0
    )
    real = functools.partial(jax.ShapeDtypeStruct, dtype=jnp.float32)
    begun, worst, asked = pl.pallas_call(
        put_own,
        out_shape=(whole_type, real((2, COLS)), real((3, 2, COLS))),
        in_specs=[hbm, vmem],
        out_specs=(hbm, vmem, vmem),
        scratch_shapes=[
            pltpu.SMEM(plan.shape, plan.dtype),
            pltpu.SemaphoreType.DMA((4,)),
            pltpu.SemaphoreType.DMA,
        ],
        compiler_params=ROOM,
        cost_estimate=cost,
    )(plan, own)
    whole, reports = pl.pallas_call(
        put_other,
        out_shape=(whole_type, real((3,))),
        in_specs=[vmem, vmem, vmem, hbm],
        out_specs=(hbm, hbm),
        scratch_shapes=[
            pltpu.SMEM((3,), jnp.float32),
            pltpu.SemaphoreType.DMA((4,)),
            pltpu.SemaphoreType.DMA,
        ],
        input_output_aliases={3: 0},
        compiler_params=ROOM,
    )(worst, asked, other, begun)
    whole = whole.reshape(rows // 8, tiles, 8, COLS).transpose(0, 2, 1, 3)
    return whole.reshape(grads.shape), reports


def solution(mesh):
    torus = Mesh(
        mesh.devices.reshape(4, 2, 4, 2, mesh.shape["gz"]),
        ("z", "core", "y", "x_lo", "x_hi"),
    )
    placed = P(("z", "core"), ("y", "x_lo"), "x_hi", None, None)
    return jax.shard_map(
        on_device,
        mesh=torus,
        in_specs=(placed, P()),
        out_specs=(placed, P()),
        check_vma=False,
    )
```

```python
import functools

import jax
import jax.numpy as jnp
from jax import lax
from jax.experimental import pallas as pl
from jax.experimental.pallas import tpu as pltpu
from jax.sharding import Mesh
from jax.sharding import PartitionSpec as P

PLANE = ("y", "z", "x_hi", "x_lo")
EVERY = ("core", *PLANE)
COLS = 128
DATA = 14
CARRIED = 16
TILES = 4 * DATA // 8
UPPER = 4
FLIP = 0b101010
SLOT = COLS // 8
ROOM = pltpu.CompilerParams(vmem_limit_bytes=8 * 2**20)


def both_ways(high, low, mean):
    return jnp.maximum(high - mean, mean - low)


def stats(values):
    total = high = low = values[0]
    for value in values[1:]:
        total = total + value
        high = jnp.maximum(high, value)
        low = jnp.minimum(low, value)
    return total, high, low


def rows_of(tiles):
    return jnp.concatenate(tiles, axis=0)


def tiles_of(rows):
    return [rows[8 * t : 8 * t + 8] for t in range(rows.shape[0] // 8)]


def across_x_hi(tiles):
    turned = {t: pltpu.roll(tiles[t], 4, 0) for t in (0, 3, 4, 5, 6)}
    first = lax.broadcasted_iota(jnp.int32, (8, COLS), 0) < 4
    return [
        jnp.where(first, turned[t + 3], turned[(t + 4) % TILES])
        for t in range(UPPER)
    ]


def across_x_lo(tiles):
    rows = rows_of(tiles)
    n = rows.shape[0]
    place = lax.broadcasted_iota(jnp.int32, rows.shape, 0)
    first = ((place >= 0) & (place < DATA)) | (
        (place >= 2 * DATA) & (place < 3 * DATA)
    )
    return tiles_of(
        jnp.where(
            first, pltpu.roll(rows, n - DATA, 0), pltpu.roll(rows, DATA, 0)
        )
    )


def most(values):
    worst = values[0]
    for value in values[1:]:
        worst = jnp.maximum(worst, value)
    return worst


def gaps(tiles, means):
    return [jnp.abs(t - m) for t, m in zip(tiles, means)]


def packed(eight):
    worst = rows_of([jnp.max(v, axis=0, keepdims=True) for v in eight])
    for apart in (64, 32, 16):
        worst = jnp.maximum(worst, pltpu.roll(worst, apart, 1))
    row = lax.broadcasted_iota(jnp.int32, worst.shape, 0)
    lane = lax.broadcasted_iota(jnp.int32, worst.shape, 1)
    return jnp.max(
        jnp.where(row == lane // SLOT, worst, 0.0), axis=0, keepdims=True
    )


def rounds(g_ref, share_ref):
    where = {
        (gx, y): (gx // 4) * 16 + y * 4 + gx % 4
        for gx in range(8)
        for y in range(4)
    }
    half = lambda tiles: [t * 0.5 for t in tiles]
    mx, dev_x = [None] * 4, []
    my_sum, y_high, y_low = [[] for _ in range(8)], [], []
    load = lambda gx, y, t: g_ref[where[gx, y], 8 * t : 8 * t + 8]

    dev_z = []
    mz_of_y = [[[] for _ in range(UPPER)] for _ in range(4)]
    mz_of_gx = [[[] for _ in range(UPPER)] for _ in range(8)]
    for y in range(4):
        x_stats = []
        for t in range(TILES):
            x_stats.append(stats([load(gx, y, t) for gx in range(8)]))
        mx[y] = [s[0] * 0.125 for s in x_stats]
        dev_x += [both_ways(s[1], s[2], m) for s, m in zip(x_stats, mx[y])]
        for gx in range(8):
            tiles = [load(gx, y, t) for t in range(TILES)]
            for t, other in enumerate(across_x_hi(tiles)):
                mean = (tiles[t] + other) * 0.5
                dev_z.append(jnp.abs(tiles[t] - mean))
                mz_of_y[y][t].append(mean)
                mz_of_gx[gx][t].append(mean)
        dev_x, dev_z = [most(dev_x)], [most(dev_z)]

    my, dev_y = [], []
    for gx in range(8):
        y_stats = [
            stats([load(gx, y, t) for y in range(4)]) for t in range(TILES)
        ]
        total = [s[0] for s in y_stats]
        my.append([(a + b) * 0.125 for a, b in zip(total, across_x_lo(total))])
        dev_y += [both_ways(s[1], s[2], m) for s, m in zip(y_stats, my[gx])]
        dev_y = [most(dev_y)]

    def with_other(tiles):
        return [(a + b) * 0.5 for a, b in zip(tiles, across_x_hi(tiles))]

    mxz = [with_other(m) for m in mx]
    myz = [with_other(m) for m in my]
    mxy = [stats([my[gx][t] for gx in range(8)])[0] * 0.125 for t in range(TILES)]
    mall = with_other(mxy)

    x_xy = most([most(gaps(mx[y], mxy)) for y in range(4)])
    x_xz = most([most(gaps(mx[y][:UPPER], mxz[y])) for y in range(4)])
    y_xy = most([most(gaps(my[gx], mxy)) for gx in range(8)])
    y_yz = most([most(gaps(my[gx][:UPPER], myz[gx])) for gx in range(8)])

    def spread_of(values, means):
        worst = []
        for t in range(UPPER):
            _, high, low = stats(values[t])
            worst.append(both_ways(high, low, means[t]))
        return most(worst)

    z_xz = most([spread_of(mz_of_y[y], mxz[y]) for y in range(4)])
    z_yz = most([spread_of(mz_of_gx[gx], myz[gx]) for gx in range(8)])
    xy_all = most(gaps(mxy[:UPPER], mall))
    xz_all = most([most(gaps(mxz[y], mall)) for y in range(4)])
    yz_all = most([most(gaps(myz[gx], mall)) for gx in range(8)])

    none = jnp.zeros((8, COLS), jnp.float32)
    slots = [dev_x[0], dev_y[0], dev_z[0]]
    slots += [none, x_xy, x_xz, y_xy, none, y_yz, z_xz, z_yz, none]
    slots += [yz_all, xz_all, xy_all, none]
    told = rows_of([packed(slots[:8]), packed(slots[8:])])
    share = jnp.concatenate([rows_of(mall[:2])[:DATA], told], axis=0)
    for i in range(share_ref.shape[0]):
        share_ref[i] = share


def begin(half_ref, out_ref, side, sems):
    count = half_ref.shape[0]
    part = count // sems.shape[0]
    copies = [
        pltpu.make_async_copy(
            half_ref.at[pl.ds(i * part, part), : DATA // 2],
            out_ref.at[pl.ds(side * count + i * part, part)],
            sems.at[i],
        )
        for i in range(sems.shape[0])
    ]
    for copy in copies:
        copy.start()
    return copies


def put_own(
    plan_ref, own_ref, out_ref, worst_ref, asked_ref, plan_here, sems, plan_sem
):
    asked = pltpu.make_async_copy(plan_ref, plan_here, plan_sem)
    asked.start()
    copies = begin(own_ref, out_ref, lax.axis_index("core"), sems)
    worst = jnp.max(own_ref[:, DATA // 2], axis=0)
    worst_ref[...] = worst
    row = lax.broadcasted_iota(jnp.int32, worst.shape, 0)
    lane = lax.broadcasted_iota(jnp.int32, worst.shape, 1)
    slot = 8 * row + lane // SLOT
    asked.wait()
    a, b, c = plan_here[0], plan_here[1], plan_here[2]
    for r, wanted in enumerate((a, 3 + 3 * a + b, 12 + c)):
        asked_ref[r] = jnp.where(slot == wanted, 1.0, 0.0)
    for copy in copies:
        copy.wait()


def put_other(
    worst_ref, asked_ref, other_ref, _, out_ref, reports_ref,
    reports_here, sems, reports_sem,
):
    copies = begin(other_ref, out_ref, 1 - lax.axis_index("core"), sems)
    worst = jnp.maximum(
        worst_ref[...], jnp.max(other_ref[:, DATA // 2], axis=0)
    )
    for r in range(3):
        wanted = asked_ref[r] > 0.0
        reports_here[r] = jnp.max(jnp.where(wanted, worst, 0.0))
    told = pltpu.make_async_copy(reports_here, reports_ref, reports_sem)
    told.start()
    for copy in (*copies, told):
        copy.wait()


def on_device(grads, plan):
    rows, width = grads.shape[-2:]
    tiles = width // COLS
    count = lax.axis_size(EVERY)
    vmem = pl.BlockSpec(memory_space=pltpu.VMEM)
    hbm = pl.BlockSpec(memory_space=pl.ANY)
    entries = grads.reshape(rows // 8, 8, tiles, COLS).transpose(0, 2, 1, 3)
    entries = entries.reshape(count, DATA // 2, 2, COLS)
    arrived = lax.all_to_all(
        entries, EVERY, 0, 0, tiled=True,
        axis_index_groups=[[i ^ FLIP for i in range(count)]],
    )
    peers = lax.axis_size(PLANE)
    share = pl.pallas_call(
        rounds,
        out_shape=jax.ShapeDtypeStruct((peers, CARRIED, COLS), jnp.float32),
        in_specs=[vmem],
        out_specs=vmem,
        compiler_params=ROOM,
    )(arrived.reshape(count // 4, 4 * DATA, COLS))
    own = lax.all_to_all(
        share, PLANE, 0, 0, tiled=True,
        axis_index_groups=[[i ^ FLIP for i in range(peers)]],
    )
    own = own.reshape(peers, CARRIED // 2, 2, COLS)
    other = lax.ppermute(own, "core", [(0, 1), (1, 0)])
    whole_type = jax.ShapeDtypeStruct((count, DATA // 2, 2, COLS), jnp.float32)
    cost = pl.CostEstimate(
        flops=10**7, bytes_accessed=own.size * 4, transcendentals=0
    )
    real = functools.partial(jax.ShapeDtypeStruct, dtype=jnp.float32)
    begun, worst, asked = pl.pallas_call(
        put_own,
        out_shape=(whole_type, real((2, COLS)), real((3, 2, COLS))),
        in_specs=[hbm, vmem],
        out_specs=(hbm, vmem, vmem),
        scratch_shapes=[
            pltpu.SMEM(plan.shape, plan.dtype),
            pltpu.SemaphoreType.DMA((4,)),
            pltpu.SemaphoreType.DMA,
        ],
        compiler_params=ROOM,
        cost_estimate=cost,
    )(plan, own)
    whole, reports = pl.pallas_call(
        put_other,
        out_shape=(whole_type, real((3,))),
        in_specs=[vmem, vmem, vmem, hbm],
        out_specs=(hbm, hbm),
        scratch_shapes=[
            pltpu.SMEM((3,), jnp.float32),
            pltpu.SemaphoreType.DMA((4,)),
            pltpu.SemaphoreType.DMA,
        ],
        input_output_aliases={3: 0},
        compiler_params=ROOM,
    )(worst, asked, other, begun)
    whole = whole.reshape(rows // 8, tiles, 8, COLS).transpose(0, 2, 1, 3)
    return whole.reshape(grads.shape), reports


def solution(mesh):
    torus = Mesh(
        mesh.devices.reshape(4, 2, 4, 2, mesh.shape["gz"]),
        ("z", "core", "y", "x_lo", "x_hi"),
    )
    placed = P(("z", "core"), ("y", "x_lo"), "x_hi", None, None)
    return jax.shard_map(
        on_device,
        mesh=torus,
        in_specs=(placed, P()),
        out_specs=(placed, P()),
        check_vma=False,
    )
```

```python
import functools

import jax
import jax.numpy as jnp
from jax import lax
from jax.experimental import pallas as pl
from jax.experimental.pallas import tpu as pltpu
from jax.sharding import Mesh
from jax.sharding import PartitionSpec as P

PLANE = ("y", "z", "x_hi", "x_lo")
FLIP = 0b101010
COLS = 128
CHIP = 28
CORE = CHIP // 2
CARRIED = 16
SIDE = 2 * CHIP // 8
ONE = 4
SLOT = COLS // 8
ROOM = pltpu.CompilerParams(vmem_limit_bytes=8 * 2**20)


def both_ways(high, low, mean):
    return jnp.maximum(high - mean, mean - low)


def most(values):
    return functools.reduce(jnp.maximum, values)


def gaps(tiles, means):
    return [jnp.abs(t - m) for t, m in zip(tiles, means)]


def stats(values):
    return (
        functools.reduce(jnp.add, values),
        functools.reduce(jnp.maximum, values),
        functools.reduce(jnp.minimum, values),
    )


def halves(tiles):
    return [(a + b) * 0.5 for a, b in zip(tiles[:SIDE], tiles[SIDE:])]


def across_x_lo(tiles):
    turned = [pltpu.roll(t, 4, 0) for t in tiles]
    first = lax.broadcasted_iota(jnp.int32, (8, COLS), 0) < 4
    return [
        jnp.where(first, turned[(t + 3) % SIDE], turned[(t + 4) % SIDE])
        for t in range(SIDE)
    ]


def over_gy(tiles):
    other = across_x_lo(tiles[:SIDE]) + across_x_lo(tiles[SIDE:])
    return [(a + b) * 0.125 for a, b in zip(tiles, other)]


def tile(ref, i, t):
    return ref[i, 8 * t : 8 * t + 8]


def tiles_of(ref, i):
    return [tile(ref, i, t) for t in range(ref.shape[1] // 8)]


def put(ref, i, tiles):
    for t, value in enumerate(tiles):
        ref[i, 8 * t : 8 * t + 8] = value


def sums(g_ref, sum_ref):
    for y in range(4):
        put(
            sum_ref,
            y,
            [
                functools.reduce(
                    jnp.add, [tile(g_ref, 4 * y + z, t) for z in range(4)]
                )
                for t in range(2 * SIDE)
            ],
        )


def alone(
    g_ref, high_ref, low_ref, mz_high_ref, mz_low_ref, my_ref, myz_ref, far_ref
):
    dev_z, z_yz = [], []
    mz_of_z = [[] for _ in range(4)]
    for y in range(4):
        high, low, mz_high, mz_low = [], [], [], []
        for t in range(SIDE):
            mz = []
            for half in (t, t + SIDE):
                values = [tile(g_ref, 4 * y + z, half) for z in range(4)]
                _, top, bottom = stats(values)
                high.append(top)
                low.append(bottom)
            for z in range(4):
                a = tile(g_ref, 4 * y + z, t)
                mean = (a + tile(g_ref, 4 * y + z, t + SIDE)) * 0.5
                dev_z.append(jnp.abs(a - mean))
                mz.append(mean)
            _, top, bottom = stats(mz)
            mz_high.append(top)
            mz_low.append(bottom)
            dev_z = [most(dev_z)]
        put(high_ref, y, high[::2] + high[1::2])
        put(low_ref, y, low[::2] + low[1::2])
        put(mz_high_ref, y, mz_high)
        put(mz_low_ref, y, mz_low)

    dev_y, y_yz = [], []
    for z in range(4):
        found = [
            stats([tile(g_ref, 4 * y + z, t) for y in range(4)])
            for t in range(2 * SIDE)
        ]
        my = over_gy([f[0] for f in found])
        myz = halves(my)
        put(my_ref, z, my)
        put(myz_ref, z, myz)
        dev_y.append(most([both_ways(f[1], f[2], m) for f, m in zip(found, my)]))
        y_yz.append(most(gaps(my[:ONE], myz)))
        for t in range(SIDE):
            mz = [
                (tile(g_ref, 4 * y + z, t) + tile(g_ref, 4 * y + z, t + SIDE))
                * 0.5
                for y in range(4)
            ]
            _, top, bottom = stats(mz)
            z_yz.append(both_ways(top, bottom, myz[t]))
        z_yz = [most(z_yz)]
    for i, worst in enumerate((dev_y, dev_z, y_yz, z_yz)):
        far_ref[i] = most(worst)


def packed(eight):
    worst = jnp.concatenate(
        [jnp.max(v, axis=0, keepdims=True) for v in eight], axis=0
    )
    for apart in (64, 32, 16):
        worst = jnp.maximum(worst, pltpu.roll(worst, apart, 1))
    row = lax.broadcasted_iota(jnp.int32, worst.shape, 0)
    lane = lax.broadcasted_iota(jnp.int32, worst.shape, 1)
    return jnp.max(
        jnp.where(row == lane // SLOT, worst, 0.0), axis=0, keepdims=True
    )


def together(
    own_ref, other_ref, high_ref, low_ref, mz_high_ref, mz_low_ref, my_ref,
    myz_ref, far_ref, share_ref,
):
    mx, mxz, dev_x, z_xz = [], [], [], []
    for y in range(4):
        mx.append(
            [
                (a + b) * 0.125
                for a, b in zip(tiles_of(own_ref, y), tiles_of(other_ref, y))
            ]
        )
        mxz.append(halves(mx[y]))
        for t in range(2 * SIDE):
            dev_x.append(
                both_ways(tile(high_ref, y, t), tile(low_ref, y, t), mx[y][t])
            )
        for t in range(SIDE):
            z_xz.append(
                both_ways(
                    tile(mz_high_ref, y, t), tile(mz_low_ref, y, t), mxz[y][t]
                )
            )
        dev_x, z_xz = [most(dev_x)], [most(z_xz)]
    mxy = over_gy(
        [
            functools.reduce(jnp.add, [mx[y][t] for y in range(4)])
            for t in range(2 * SIDE)
        ]
    )
    mall = halves(mxy)
    once = (*range(ONE), *range(SIDE, SIDE + ONE))
    x_xy = most([most(gaps(mx[y], mxy)) for y in range(4)])
    x_xz = most([most(gaps(mx[y][:SIDE], mxz[y])) for y in range(4)])
    y_xy = most(
        [jnp.abs(tile(my_ref, z, t) - mxy[t]) for z in range(4) for t in once]
    )
    xy_all = most(gaps(mxy[:ONE], mall))
    xz_all = most([most(gaps(mxz[y], mall)) for y in range(4)])
    yz_all = most(
        [
            jnp.abs(tile(myz_ref, z, t) - mall[t])
            for z in range(4)
            for t in range(ONE)
        ]
    )
    none = jnp.zeros((8, COLS), jnp.float32)
    dev_y, dev_z, y_yz, z_yz = (far_ref[i] for i in range(4))
    slots = [dev_x[0], dev_y, dev_z]
    slots += [none, x_xy, x_xz, y_xy, none, y_yz]
    slots += [z_xz[0], z_yz, none]
    slots += [yz_all, xz_all, xy_all, none]
    mean = jnp.concatenate(mall[:ONE], axis=0)
    mine = jnp.where(
        lax.axis_index("core") == 0, mean[:CORE], mean[CORE : 2 * CORE]
    )
    share = jnp.concatenate([mine, packed(slots[:8]), packed(slots[8:])], axis=0)
    for i in range(share_ref.shape[0]):
        share_ref[i] = share


def begin(half_ref, out_ref, side, sems):
    count = half_ref.shape[0]
    part = count // sems.shape[0]
    copies = [
        pltpu.make_async_copy(
            half_ref.at[pl.ds(i * part, part), : CORE // 2],
            out_ref.at[pl.ds(i * part, part), side],
            sems.at[i],
        )
        for i in range(sems.shape[0])
    ]
    for copy in copies:
        copy.start()
    return copies


def put_own(
    plan_ref, own_ref, out_ref, worst_ref, asked_ref, plan_here, sems, plan_sem
):
    asked = pltpu.make_async_copy(plan_ref, plan_here, plan_sem)
    asked.start()
    copies = begin(own_ref, out_ref, lax.axis_index("core"), sems)
    worst = jnp.max(own_ref[:, CORE // 2], axis=0)
    worst_ref[...] = worst
    row = lax.broadcasted_iota(jnp.int32, worst.shape, 0)
    lane = lax.broadcasted_iota(jnp.int32, worst.shape, 1)
    slot = 8 * row + lane // SLOT
    asked.wait()
    a, b, c = plan_here[0], plan_here[1], plan_here[2]
    for r, wanted in enumerate((a, 3 + 3 * a + b, 12 + c)):
        asked_ref[r] = jnp.where(slot == wanted, 1.0, 0.0)
    for copy in copies:
        copy.wait()


def put_other(
    worst_ref, asked_ref, other_ref, _, out_ref, reports_ref,
    reports_here, sems, reports_sem,
):
    copies = begin(other_ref, out_ref, 1 - lax.axis_index("core"), sems)
    worst = jnp.maximum(
        worst_ref[...], jnp.max(other_ref[:, CORE // 2], axis=0)
    )
    for r in range(3):
        wanted = asked_ref[r] > 0.0
        reports_here[r] = jnp.max(jnp.where(wanted, worst, 0.0))
    told = pltpu.make_async_copy(reports_here, reports_ref, reports_sem)
    told.start()
    for copy in (*copies, told):
        copy.wait()


def on_device(grads, plan):
    rows, width = grads.shape[-2:]
    tiles = width // COLS
    chips = lax.axis_size(PLANE)
    real = functools.partial(jax.ShapeDtypeStruct, dtype=jnp.float32)
    vmem = pl.BlockSpec(memory_space=pltpu.VMEM)
    hbm = pl.BlockSpec(memory_space=pl.ANY)
    kernel = functools.partial(pl.pallas_call, compiler_params=ROOM)
    under_swap = pl.CostEstimate(
        flops=10**7, bytes_accessed=grads.size * 4, transcendentals=0
    )
    cores = [(0, 1), (1, 0)]
    members = [[i ^ FLIP for i in range(chips)]]

    entries = grads.reshape(rows // 8, 8, tiles, COLS).transpose(0, 2, 1, 3)
    entries = entries.reshape(chips, CHIP // 2, 2, COLS)
    arrived = lax.all_to_all(
        entries, PLANE, 0, 0, tiled=True, axis_index_groups=members
    ).reshape(chips // 4, 4 * CHIP, COLS)
    four, side = real((4, 4 * CHIP, COLS)), real((4, 2 * CHIP, COLS))
    own_sum = kernel(sums, out_shape=four, in_specs=[vmem], out_specs=vmem)(
        arrived
    )
    other_sum = lax.ppermute(own_sum, "core", cores)
    local = kernel(
        alone,
        out_shape=(four, four, side, side, four, side, real((4, 8, COLS))),
        in_specs=[vmem],
        out_specs=(vmem,) * 7,
        cost_estimate=under_swap,
    )(arrived)
    share = kernel(
        together,
        out_shape=real((chips, CARRIED, COLS)),
        in_specs=[vmem] * 9,
        out_specs=vmem,
    )(own_sum, other_sum, *local)
    own = lax.all_to_all(
        share, PLANE, 0, 0, tiled=True, axis_index_groups=members
    ).reshape(chips, CARRIED // 2, 2, COLS)
    other = lax.ppermute(own, "core", cores)
    whole = real((chips, 2, CORE // 2, 2, COLS))
    begun, worst, asked = kernel(
        put_own,
        out_shape=(whole, real((2, COLS)), real((3, 2, COLS))),
        in_specs=[hbm, vmem],
        out_specs=(hbm, vmem, vmem),
        scratch_shapes=[
            pltpu.SMEM(plan.shape, plan.dtype),
            pltpu.SemaphoreType.DMA((4,)),
            pltpu.SemaphoreType.DMA,
        ],
        cost_estimate=under_swap,
    )(plan, own)
    whole, reports = kernel(
        put_other,
        out_shape=(whole, real((3,))),
        in_specs=[vmem, vmem, vmem, hbm],
        out_specs=(hbm, hbm),
        scratch_shapes=[
            pltpu.SMEM((3,), jnp.float32),
            pltpu.SemaphoreType.DMA((4,)),
            pltpu.SemaphoreType.DMA,
        ],
        input_output_aliases={3: 0},
    )(worst, asked, other, begun)
    whole = whole.reshape(rows // 8, tiles, 8, COLS).transpose(0, 2, 1, 3)
    return whole.reshape(grads.shape), reports


def solution(mesh):
    torus = Mesh(
        mesh.devices.reshape(4, 2, 4, 2, mesh.shape["gz"]),
        ("z", "core", "y", "x_lo", "x_hi"),
    )
    placed = P(("z", "core"), ("y", "x_lo"), "x_hi", None, None)
    return jax.shard_map(
        on_device,
        mesh=torus,
        in_specs=(placed, P()),
        out_specs=(placed, P()),
        check_vma=False,
    )
```

```python
import functools

import jax
import jax.numpy as jnp
from jax import lax
from jax.experimental import pallas as pl
from jax.experimental.pallas import tpu as pltpu
from jax.sharding import Mesh
from jax.sharding import PartitionSpec as P

PLANE = ("y", "z", "x_hi", "x_lo")
YZ_ORDER, X_ORDER = (2, 0, 1, 3), (2, 3, 0, 1)
COLS = 128
CHIP = 28
CORE = CHIP // 2
CARRIED = 16
SIDE = 2 * CHIP // 8
ONE = 4
ROOM = pltpu.CompilerParams(vmem_limit_bytes=8 * 2**20)


def both_ways(high, low, mean):
    return jnp.maximum(high - mean, mean - low)


def most(values):
    return functools.reduce(jnp.maximum, values)


def gaps(tiles, means):
    return [jnp.abs(t - m) for t, m in zip(tiles, means)]


def stats(values):
    return (
        functools.reduce(jnp.add, values),
        functools.reduce(jnp.maximum, values),
        functools.reduce(jnp.minimum, values),
    )


def halves(tiles):
    return [(a + b) * 0.5 for a, b in zip(tiles[:SIDE], tiles[SIDE:])]


def across_x_lo(tiles):
    turned = [pltpu.roll(t, 4, 0) for t in tiles]
    first = lax.broadcasted_iota(jnp.int32, (8, COLS), 0) < 4
    return [
        jnp.where(first, turned[(t + 3) % SIDE], turned[(t + 4) % SIDE])
        for t in range(SIDE)
    ]


def over_gy(tiles):
    other = across_x_lo(tiles[:SIDE]) + across_x_lo(tiles[SIDE:])
    return [(a + b) * 0.125 for a, b in zip(tiles, other)]


def tile(ref, i, t):
    return ref[i, 8 * t : 8 * t + 8]


def tiles_of(ref, i):
    return [tile(ref, i, t) for t in range(ref.shape[1] // 8)]


def put(ref, i, tiles):
    for t, value in enumerate(tiles):
        ref[i, 8 * t : 8 * t + 8] = value


def sums(g_ref, sum_ref):
    for y in range(4):
        put(
            sum_ref,
            y,
            [
                functools.reduce(
                    jnp.add, [tile(g_ref, 4 * y + z, t) for z in range(4)]
                )
                for t in range(2 * SIDE)
            ],
        )


def alone(
    plan_ref, g_ref, high_ref, low_ref, mz_high_ref, mz_low_ref, my_ref,
    myz_ref, far_ref, mask_ref, plan_here, plan_sem,
):
    asked = pltpu.make_async_copy(plan_ref, plan_here, plan_sem)
    asked.start()
    dev_z, z_yz = [], []
    mz_of_z = [[] for _ in range(4)]
    for y in range(4):
        high, low, mz_high, mz_low = [], [], [], []
        for t in range(SIDE):
            mz = []
            for half in (t, t + SIDE):
                values = [tile(g_ref, 4 * y + z, half) for z in range(4)]
                _, top, bottom = stats(values)
                high.append(top)
                low.append(bottom)
            for z in range(4):
                a = tile(g_ref, 4 * y + z, t)
                mean = (a + tile(g_ref, 4 * y + z, t + SIDE)) * 0.5
                dev_z.append(jnp.abs(a - mean))
                mz.append(mean)
            _, top, bottom = stats(mz)
            mz_high.append(top)
            mz_low.append(bottom)
            dev_z = [most(dev_z)]
        put(high_ref, y, high[::2] + high[1::2])
        put(low_ref, y, low[::2] + low[1::2])
        put(mz_high_ref, y, mz_high)
        put(mz_low_ref, y, mz_low)

    dev_y, y_yz = [], []
    for z in range(4):
        found = [
            stats([tile(g_ref, 4 * y + z, t) for y in range(4)])
            for t in range(2 * SIDE)
        ]
        my = over_gy([f[0] for f in found])
        myz = halves(my)
        put(my_ref, z, my)
        put(myz_ref, z, myz)
        dev_y.append(most([both_ways(f[1], f[2], m) for f, m in zip(found, my)]))
        y_yz.append(most(gaps(my[:ONE], myz)))
        for t in range(SIDE):
            mz = [
                (tile(g_ref, 4 * y + z, t) + tile(g_ref, 4 * y + z, t + SIDE))
                * 0.5
                for y in range(4)
            ]
            _, top, bottom = stats(mz)
            z_yz.append(both_ways(top, bottom, myz[t]))
        z_yz = [most(z_yz)]
    for i, worst in enumerate((dev_y, dev_z, y_yz, z_yz)):
        far_ref[i] = most(worst)
    asked.wait()
    wanted(plan_here, mask_ref)


def wanted(plan_ref, mask_ref):
    a, b, c = plan_ref[0], plan_ref[1], plan_ref[2]
    for i in range(mask_ref.shape[0]):
        asked = (i == a) | (i == 3 + 3 * a + b) | (i == 12 + c)
        mask_ref[i] = jnp.full((8, COLS), jnp.where(asked, 1.0, 0.0))


def folded(mask_ref, choices):
    worst = most(
        [jnp.where(mask_ref[i] > 0.0, v, 0.0) for i, v in choices.items()]
    )
    worst = jnp.max(worst, axis=0, keepdims=True)
    return jnp.maximum(worst, pltpu.roll(worst, COLS // 2, 1))


def together(
    own_ref, other_ref, high_ref, low_ref, mz_high_ref, mz_low_ref, my_ref,
    myz_ref, far_ref, mask_ref, share_ref,
):
    mx, mxz, dev_x, z_xz = [], [], [], []
    for y in range(4):
        mx.append(
            [
                (a + b) * 0.125
                for a, b in zip(tiles_of(own_ref, y), tiles_of(other_ref, y))
            ]
        )
        mxz.append(halves(mx[y]))
        for t in range(2 * SIDE):
            dev_x.append(
                both_ways(tile(high_ref, y, t), tile(low_ref, y, t), mx[y][t])
            )
        for t in range(SIDE):
            z_xz.append(
                both_ways(
                    tile(mz_high_ref, y, t), tile(mz_low_ref, y, t), mxz[y][t]
                )
            )
        dev_x, z_xz = [most(dev_x)], [most(z_xz)]
    mxy = over_gy(
        [
            functools.reduce(jnp.add, [mx[y][t] for y in range(4)])
            for t in range(2 * SIDE)
        ]
    )
    mall = halves(mxy)
    once = (*range(ONE), *range(SIDE, SIDE + ONE))
    x_xy = most([most(gaps(mx[y], mxy)) for y in range(4)])
    x_xz = most([most(gaps(mx[y][:SIDE], mxz[y])) for y in range(4)])
    y_xy = most(
        [jnp.abs(tile(my_ref, z, t) - mxy[t]) for z in range(4) for t in once]
    )
    xy_all = most(gaps(mxy[:ONE], mall))
    xz_all = most([most(gaps(mxz[y], mall)) for y in range(4)])
    yz_all = most(
        [
            jnp.abs(tile(myz_ref, z, t) - mall[t])
            for z in range(4)
            for t in range(ONE)
        ]
    )
    dev_y, dev_z, y_yz, z_yz = (far_ref[i] for i in range(4))
    first = folded(mask_ref, {0: dev_x[0], 1: dev_y, 2: dev_z})
    second = folded(
        mask_ref,
        {4: x_xy, 5: x_xz, 6: y_xy, 8: y_yz, 9: z_xz[0], 10: z_yz},
    )
    third = folded(mask_ref, {12: yz_all, 13: xz_all, 14: xy_all})
    lane = lax.broadcasted_iota(jnp.int32, (1, COLS), 1)
    told = [jnp.where(lane < COLS // 2, first, second), third]
    mean = jnp.concatenate(mall[:ONE], axis=0)
    mine = jnp.where(
        lax.axis_index("core") == 0, mean[:CORE], mean[CORE : 2 * CORE]
    )
    share = jnp.concatenate([mine, *told], axis=0)
    for i in range(share_ref.shape[0]):
        share_ref[i] = share


def begin(half_ref, out_ref, side, sems):
    count = half_ref.shape[0]
    part = count // sems.shape[0]
    copies = [
        pltpu.make_async_copy(
            half_ref.at[pl.ds(i * part, part), : CORE // 2],
            out_ref.at[pl.ds(i * part, part), side],
            sems.at[i],
        )
        for i in range(sems.shape[0])
    ]
    for copy in copies:
        copy.start()
    return copies


def put_own(own_ref, out_ref, worst_ref, sems):
    copies = begin(own_ref, out_ref, lax.axis_index("core"), sems)
    worst_ref[...] = jnp.max(own_ref[:, CORE // 2], axis=0)
    for copy in copies:
        copy.wait()


def put_other(
    worst_ref, other_ref, _, out_ref, reports_ref,
    reports_here, sems, reports_sem,
):
    copies = begin(other_ref, out_ref, 1 - lax.axis_index("core"), sems)
    worst = jnp.maximum(
        worst_ref[...], jnp.max(other_ref[:, CORE // 2], axis=0)
    )
    lane = lax.broadcasted_iota(jnp.int32, (1, COLS), 1)
    first = lane < COLS // 2
    reports_here[0] = jnp.max(jnp.where(first, worst[:1], 0.0))
    reports_here[1] = jnp.max(jnp.where(first, 0.0, worst[:1]))
    reports_here[2] = jnp.max(worst[1:])
    told = pltpu.make_async_copy(reports_here, reports_ref, reports_sem)
    told.start()
    for copy in (*copies, told):
        copy.wait()


def on_device(grads, plan):
    rows, width = grads.shape[-2:]
    tiles = width // COLS
    chips = lax.axis_size(PLANE)
    real = functools.partial(jax.ShapeDtypeStruct, dtype=jnp.float32)
    vmem = pl.BlockSpec(memory_space=pltpu.VMEM)
    hbm = pl.BlockSpec(memory_space=pl.ANY)
    kernel = functools.partial(pl.pallas_call, compiler_params=ROOM)
    under_swap = pl.CostEstimate(
        flops=10**7, bytes_accessed=grads.size * 4, transcendentals=0
    )
    cores = [(0, 1), (1, 0)]
    members = [
        [16 * y + 4 * z + x for y in YZ_ORDER for z in YZ_ORDER for x in X_ORDER]
    ]

    entries = grads.reshape(rows // 8, 8, tiles, COLS).transpose(0, 2, 1, 3)
    entries = entries.reshape(chips, CHIP // 2, 2, COLS)
    arrived = lax.all_to_all(
        entries, PLANE, 0, 0, tiled=True, axis_index_groups=members
    ).reshape(chips // 4, 4 * CHIP, COLS)
    four, side = real((4, 4 * CHIP, COLS)), real((4, 2 * CHIP, COLS))
    own_sum = kernel(sums, out_shape=four, in_specs=[vmem], out_specs=vmem)(
        arrived
    )
    other_sum = lax.ppermute(own_sum, "core", cores)
    local = kernel(
        alone,
        out_shape=(
            *(four, four, side, side, four, side),
            real((4, 8, COLS)),
            real((15, 8, COLS)),
        ),
        in_specs=[hbm, vmem],
        out_specs=(vmem,) * 8,
        scratch_shapes=[
            pltpu.SMEM(plan.shape, plan.dtype),
            pltpu.SemaphoreType.DMA,
        ],
        cost_estimate=under_swap,
    )(plan, arrived)
    share = kernel(
        together,
        out_shape=real((chips, CARRIED, COLS)),
        in_specs=[vmem] * 10,
        out_specs=vmem,
    )(own_sum, other_sum, *local)
    own = lax.all_to_all(
        share, PLANE, 0, 0, tiled=True, axis_index_groups=members
    ).reshape(chips, CARRIED // 2, 2, COLS)
    other = lax.ppermute(own, "core", cores)
    whole = real((chips, 2, CORE // 2, 2, COLS))
    begun, worst = kernel(
        put_own,
        out_shape=(whole, real((2, COLS))),
        in_specs=[vmem],
        out_specs=(hbm, vmem),
        scratch_shapes=[pltpu.SemaphoreType.DMA((2,))],
        cost_estimate=under_swap,
    )(own)
    whole, reports = kernel(
        put_other,
        out_shape=(whole, real((3,))),
        in_specs=[vmem, vmem, hbm],
        out_specs=(hbm, hbm),
        scratch_shapes=[
            pltpu.SMEM((3,), jnp.float32),
            pltpu.SemaphoreType.DMA((2,)),
            pltpu.SemaphoreType.DMA,
        ],
        input_output_aliases={2: 0},
    )(worst, other, begun)
    whole = whole.reshape(rows // 8, tiles, 8, COLS).transpose(0, 2, 1, 3)
    return whole.reshape(grads.shape), reports


def solution(mesh):
    torus = Mesh(
        mesh.devices.reshape(4, 2, 4, 2, mesh.shape["gz"]),
        ("z", "core", "y", "x_lo", "x_hi"),
    )
    placed = P(("z", "core"), ("y", "x_lo"), "x_hi", None, None)
    return jax.shard_map(
        on_device,
        mesh=torus,
        in_specs=(placed, P()),
        out_specs=(placed, P()),
        check_vma=False,
    )
```

```python
import functools

import jax
import jax.numpy as jnp
from jax import lax
from jax.experimental import pallas as pl
from jax.experimental.pallas import tpu as pltpu
from jax.sharding import Mesh
from jax.sharding import PartitionSpec as P

PLANE = ("z", "y", "x_hi", "x_lo")
YZ_ORDER, X_ORDER = (2, 0, 1, 3), (2, 3, 0, 1)
COLS = 128
CHIP = 28
CORE = CHIP // 2
CARRIED = 16
SIDE = 2 * CHIP // 8
ONE = 4
ROOM = pltpu.CompilerParams(vmem_limit_bytes=8 * 2**20)


def both_ways(high, low, mean):
    return jnp.maximum(high - mean, mean - low)


def most(values):
    return functools.reduce(jnp.maximum, values)


def gaps(tiles, means):
    return [jnp.abs(t - m) for t, m in zip(tiles, means)]


def stats(values):
    return (
        functools.reduce(jnp.add, values),
        functools.reduce(jnp.maximum, values),
        functools.reduce(jnp.minimum, values),
    )


def halves(tiles):
    return [(a + b) * 0.5 for a, b in zip(tiles[:SIDE], tiles[SIDE:])]


def across_x_lo(tiles):
    turned = [pltpu.roll(t, 4, 0) for t in tiles]
    first = lax.broadcasted_iota(jnp.int32, (8, COLS), 0) < 4
    return [
        jnp.where(first, turned[(t + 3) % SIDE], turned[(t + 4) % SIDE])
        for t in range(SIDE)
    ]


def over_gy(tiles):
    other = across_x_lo(tiles[:SIDE]) + across_x_lo(tiles[SIDE:])
    return [(a + b) * 0.125 for a, b in zip(tiles, other)]


def tile(ref, i, t):
    return ref[i, 8 * t : 8 * t + 8]


def tiles_of(ref, i):
    return [tile(ref, i, t) for t in range(ref.shape[1] // 8)]


def put(ref, i, tiles):
    for t, value in enumerate(tiles):
        ref[i, 8 * t : 8 * t + 8] = value


def sums(g_ref, sum_ref):
    for y in range(4):
        put(
            sum_ref,
            y,
            [
                functools.reduce(
                    jnp.add, [tile(g_ref, 4 * z + y, t) for z in range(4)]
                )
                for t in range(2 * SIDE)
            ],
        )


def alone(
    g_ref, high_ref, low_ref, mz_high_ref, mz_low_ref, my_ref, myz_ref, far_ref
):
    dev_z, z_yz = [], []
    mz_of_z = [[] for _ in range(4)]
    for y in range(4):
        high, low, mz_high, mz_low = [], [], [], []
        for t in range(SIDE):
            mz = []
            for half in (t, t + SIDE):
                values = [tile(g_ref, 4 * z + y, half) for z in range(4)]
                _, top, bottom = stats(values)
                high.append(top)
                low.append(bottom)
            for z in range(4):
                a = tile(g_ref, 4 * z + y, t)
                mean = (a + tile(g_ref, 4 * z + y, t + SIDE)) * 0.5
                dev_z.append(jnp.abs(a - mean))
                mz.append(mean)
            _, top, bottom = stats(mz)
            mz_high.append(top)
            mz_low.append(bottom)
            dev_z = [most(dev_z)]
        put(high_ref, y, high[::2] + high[1::2])
        put(low_ref, y, low[::2] + low[1::2])
        put(mz_high_ref, y, mz_high)
        put(mz_low_ref, y, mz_low)

    dev_y, y_yz = [], []
    for z in range(4):
        found = [
            stats([tile(g_ref, 4 * z + y, t) for y in range(4)])
            for t in range(2 * SIDE)
        ]
        my = over_gy([f[0] for f in found])
        myz = halves(my)
        put(my_ref, z, my)
        put(myz_ref, z, myz)
        dev_y.append(most([both_ways(f[1], f[2], m) for f, m in zip(found, my)]))
        y_yz.append(most(gaps(my[:ONE], myz)))
        for t in range(SIDE):
            mz = [
                (tile(g_ref, 4 * z + y, t) + tile(g_ref, 4 * z + y, t + SIDE))
                * 0.5
                for y in range(4)
            ]
            _, top, bottom = stats(mz)
            z_yz.append(both_ways(top, bottom, myz[t]))
        z_yz = [most(z_yz)]
    for i, worst in enumerate((dev_y, dev_z, y_yz, z_yz)):
        far_ref[i] = most(worst)


def wanted(plan_ref, mask_ref, plan_here, plan_sem):
    asked = pltpu.make_async_copy(plan_ref, plan_here, plan_sem)
    asked.start()
    asked.wait()
    a, b, c = plan_here[0], plan_here[1], plan_here[2]
    for i in range(mask_ref.shape[0]):
        asked = (i == a) | (i == 3 + 3 * a + b) | (i == 12 + c)
        mask_ref[i] = jnp.full((8, COLS), jnp.where(asked, 1.0, 0.0))


def folded(mask_ref, choices):
    worst = most(
        [jnp.where(mask_ref[i] > 0.0, v, 0.0) for i, v in choices.items()]
    )
    worst = jnp.max(worst, axis=0, keepdims=True)
    return jnp.maximum(worst, pltpu.roll(worst, COLS // 2, 1))


def together(
    own_ref, other_ref, high_ref, low_ref, mz_high_ref, mz_low_ref, my_ref,
    myz_ref, far_ref, mask_ref, share_ref,
):
    mx, mxz, dev_x, z_xz = [], [], [], []
    for y in range(4):
        mx.append(
            [
                (a + b) * 0.125
                for a, b in zip(tiles_of(own_ref, y), tiles_of(other_ref, y))
            ]
        )
        mxz.append(halves(mx[y]))
        for t in range(2 * SIDE):
            dev_x.append(
                both_ways(tile(high_ref, y, t), tile(low_ref, y, t), mx[y][t])
            )
        for t in range(SIDE):
            z_xz.append(
                both_ways(
                    tile(mz_high_ref, y, t), tile(mz_low_ref, y, t), mxz[y][t]
                )
            )
        dev_x, z_xz = [most(dev_x)], [most(z_xz)]
    mxy = over_gy(
        [
            functools.reduce(jnp.add, [mx[y][t] for y in range(4)])
            for t in range(2 * SIDE)
        ]
    )
    mall = halves(mxy)
    once = (*range(ONE), *range(SIDE, SIDE + ONE))
    x_xy = most([most(gaps(mx[y], mxy)) for y in range(4)])
    x_xz = most([most(gaps(mx[y][:SIDE], mxz[y])) for y in range(4)])
    y_xy = most(
        [jnp.abs(tile(my_ref, z, t) - mxy[t]) for z in range(4) for t in once]
    )
    xy_all = most(gaps(mxy[:ONE], mall))
    xz_all = most([most(gaps(mxz[y], mall)) for y in range(4)])
    yz_all = most(
        [
            jnp.abs(tile(myz_ref, z, t) - mall[t])
            for z in range(4)
            for t in range(ONE)
        ]
    )
    dev_y, dev_z, y_yz, z_yz = (far_ref[i] for i in range(4))
    first = folded(mask_ref, {0: dev_x[0], 1: dev_y, 2: dev_z})
    second = folded(
        mask_ref,
        {4: x_xy, 5: x_xz, 6: y_xy, 8: y_yz, 9: z_xz[0], 10: z_yz},
    )
    third = folded(mask_ref, {12: yz_all, 13: xz_all, 14: xy_all})
    lane = lax.broadcasted_iota(jnp.int32, (1, COLS), 1)
    told = [jnp.where(lane < COLS // 2, first, second), third]
    mean = jnp.concatenate(mall[:ONE], axis=0)
    mine = jnp.where(
        lax.axis_index("core") == 0, mean[:CORE], mean[CORE : 2 * CORE]
    )
    share = jnp.concatenate([mine, *told], axis=0)
    for i in range(share_ref.shape[0]):
        share_ref[i] = share


def begin(half_ref, out_ref, side, sems):
    count = half_ref.shape[0]
    part = count // sems.shape[0]
    copies = [
        pltpu.make_async_copy(
            half_ref.at[pl.ds(i * part, part), : CORE // 2],
            out_ref.at[pl.ds(i * part, part), side],
            sems.at[i],
        )
        for i in range(sems.shape[0])
    ]
    for copy in copies:
        copy.start()
    return copies


def put_own(own_ref, out_ref, worst_ref, sems):
    copies = begin(own_ref, out_ref, lax.axis_index("core"), sems)
    worst_ref[...] = jnp.max(own_ref[:, CORE // 2], axis=0)
    for copy in copies:
        copy.wait()


def put_other(
    worst_ref, other_ref, _, out_ref, reports_ref,
    reports_here, sems, reports_sem,
):
    copies = begin(other_ref, out_ref, 1 - lax.axis_index("core"), sems)
    worst = jnp.maximum(
        worst_ref[...], jnp.max(other_ref[:, CORE // 2], axis=0)
    )
    lane = lax.broadcasted_iota(jnp.int32, (1, COLS), 1)
    first = lane < COLS // 2
    reports_here[0] = jnp.max(jnp.where(first, worst[:1], 0.0))
    reports_here[1] = jnp.max(jnp.where(first, 0.0, worst[:1]))
    reports_here[2] = jnp.max(worst[1:])
    told = pltpu.make_async_copy(reports_here, reports_ref, reports_sem)
    told.start()
    for copy in (*copies, told):
        copy.wait()


def on_device(grads, plan):
    rows, width = grads.shape[-2:]
    tiles = width // COLS
    chips = lax.axis_size(PLANE)
    real = functools.partial(jax.ShapeDtypeStruct, dtype=jnp.float32)
    vmem = pl.BlockSpec(memory_space=pltpu.VMEM)
    hbm = pl.BlockSpec(memory_space=pl.ANY)
    kernel = functools.partial(pl.pallas_call, compiler_params=ROOM)
    under_swap = pl.CostEstimate(
        flops=10**7, bytes_accessed=grads.size * 4, transcendentals=0
    )
    cores = [(0, 1), (1, 0)]
    members = [
        [16 * z + 4 * y + x for z in YZ_ORDER for y in YZ_ORDER for x in X_ORDER]
    ]

    entries = grads.reshape(rows // 8, 8, tiles, COLS).transpose(0, 2, 1, 3)
    entries = entries.reshape(chips, CHIP // 2, 2, COLS)
    arrived = lax.all_to_all(
        entries, PLANE, 0, 0, tiled=True, axis_index_groups=members
    ).reshape(chips // 4, 4 * CHIP, COLS)
    four, side = real((4, 4 * CHIP, COLS)), real((4, 2 * CHIP, COLS))
    own_sum = kernel(sums, out_shape=four, in_specs=[vmem], out_specs=vmem)(
        arrived
    )
    other_sum = lax.ppermute(own_sum, "core", cores)
    local = kernel(
        alone,
        out_shape=(
            *(four, four, side, side, four, side),
            real((4, 8, COLS)),
        ),
        in_specs=[vmem],
        out_specs=(vmem,) * 7,
        cost_estimate=under_swap,
    )(arrived)
    mask = kernel(
        wanted,
        out_shape=real((15, 8, COLS)),
        in_specs=[hbm],
        out_specs=vmem,
        scratch_shapes=[
            pltpu.SMEM(plan.shape, plan.dtype),
            pltpu.SemaphoreType.DMA,
        ],
        cost_estimate=under_swap,
    )(plan)
    share = kernel(
        together,
        out_shape=real((chips, CARRIED, COLS)),
        in_specs=[vmem] * 10,
        out_specs=vmem,
    )(own_sum, other_sum, *local, mask)
    own = lax.all_to_all(
        share, PLANE, 0, 0, tiled=True, axis_index_groups=members
    ).reshape(chips, CARRIED // 2, 2, COLS)
    other = lax.ppermute(own, "core", cores)
    whole = real((chips, 2, CORE // 2, 2, COLS))
    begun, worst = kernel(
        put_own,
        out_shape=(whole, real((2, COLS))),
        in_specs=[vmem],
        out_specs=(hbm, vmem),
        scratch_shapes=[pltpu.SemaphoreType.DMA((2,))],
        cost_estimate=under_swap,
    )(own)
    whole, reports = kernel(
        put_other,
        out_shape=(whole, real((3,))),
        in_specs=[vmem, vmem, hbm],
        out_specs=(hbm, hbm),
        scratch_shapes=[
            pltpu.SMEM((3,), jnp.float32),
            pltpu.SemaphoreType.DMA((2,)),
            pltpu.SemaphoreType.DMA,
        ],
        input_output_aliases={2: 0},
    )(worst, other, begun)
    whole = whole.reshape(rows // 8, tiles, 8, COLS).transpose(0, 2, 1, 3)
    return whole.reshape(grads.shape), reports


def solution(mesh):
    torus = Mesh(
        mesh.devices.reshape(4, 2, 4, 2, mesh.shape["gz"]),
        ("z", "core", "y", "x_lo", "x_hi"),
    )
    placed = P(("z", "core"), ("y", "x_lo"), "x_hi", None, None)
    return jax.shard_map(
        on_device,
        mesh=torus,
        in_specs=(placed, P()),
        out_specs=(placed, P()),
        check_vma=False,
    )
```

```python
import functools

import jax
import jax.numpy as jnp
from jax import lax
from jax.experimental import pallas as pl
from jax.experimental.pallas import tpu as pltpu
from jax.sharding import Mesh
from jax.sharding import PartitionSpec as P

PLANE = ("z", "y", "x_hi", "x_lo")
YZ_ORDER, X_ORDER = (2, 0, 1, 3), (2, 3, 0, 1)
COLS = 128
CHIP = 28
CORE = CHIP // 2
CARRIED = 16
SIDE = 2 * CHIP // 8
ONE = 4
ROOM = pltpu.CompilerParams(vmem_limit_bytes=8 * 2**20)


def both_ways(high, low, mean):
    return jnp.maximum(high - mean, mean - low)


def most(values):
    return functools.reduce(jnp.maximum, values)


def gaps(tiles, means):
    return [jnp.abs(t - m) for t, m in zip(tiles, means)]


def stats(values):
    return (
        functools.reduce(jnp.add, values),
        functools.reduce(jnp.maximum, values),
        functools.reduce(jnp.minimum, values),
    )


def halves(tiles):
    return [(a + b) * 0.5 for a, b in zip(tiles[:SIDE], tiles[SIDE:])]


def across_x_lo(tiles):
    turned = [pltpu.roll(t, 4, 0) for t in tiles]
    first = lax.broadcasted_iota(jnp.int32, (8, COLS), 0) < 4
    return [
        jnp.where(first, turned[(t + 3) % SIDE], turned[(t + 4) % SIDE])
        for t in range(SIDE)
    ]


def over_gy(tiles):
    other = across_x_lo(tiles[:SIDE]) + across_x_lo(tiles[SIDE:])
    return [(a + b) * 0.125 for a, b in zip(tiles, other)]


def tile(ref, i, t):
    return ref[i, 8 * t : 8 * t + 8]


def tiles_of(ref, i):
    return [tile(ref, i, t) for t in range(ref.shape[1] // 8)]


def put(ref, i, tiles):
    for t, value in enumerate(tiles):
        ref[i, 8 * t : 8 * t + 8] = value


def sums(g_ref, sum_ref):
    for y in range(4):
        put(
            sum_ref,
            y,
            [
                functools.reduce(
                    jnp.add, [tile(g_ref, 4 * z + y, t) for z in range(4)]
                )
                for t in range(2 * SIDE)
            ],
        )


def alone(
    g_ref, high_ref, low_ref, mz_high_ref, mz_low_ref, my_ref, myz_ref, far_ref
):
    dev_z, z_yz = [], []
    mz_of_z = [[] for _ in range(4)]
    for y in range(4):
        high, low, mz_high, mz_low = [], [], [], []
        for t in range(SIDE):
            mz = []
            for half in (t, t + SIDE):
                values = [tile(g_ref, 4 * z + y, half) for z in range(4)]
                _, top, bottom = stats(values)
                high.append(top)
                low.append(bottom)
            for z in range(4):
                a = tile(g_ref, 4 * z + y, t)
                mean = (a + tile(g_ref, 4 * z + y, t + SIDE)) * 0.5
                dev_z.append(jnp.abs(a - mean))
                mz.append(mean)
            _, top, bottom = stats(mz)
            mz_high.append(top)
            mz_low.append(bottom)
            dev_z = [most(dev_z)]
        put(high_ref, y, high[::2] + high[1::2])
        put(low_ref, y, low[::2] + low[1::2])
        put(mz_high_ref, y, mz_high)
        put(mz_low_ref, y, mz_low)

    dev_y, y_yz = [], []
    for z in range(4):
        found = [
            stats([tile(g_ref, 4 * z + y, t) for y in range(4)])
            for t in range(2 * SIDE)
        ]
        my = over_gy([f[0] for f in found])
        myz = halves(my)
        put(my_ref, z, my)
        put(myz_ref, z, myz)
        dev_y.append(most([both_ways(f[1], f[2], m) for f, m in zip(found, my)]))
        y_yz.append(most(gaps(my[:ONE], myz)))
        for t in range(SIDE):
            mz = [
                (tile(g_ref, 4 * z + y, t) + tile(g_ref, 4 * z + y, t + SIDE))
                * 0.5
                for y in range(4)
            ]
            _, top, bottom = stats(mz)
            z_yz.append(both_ways(top, bottom, myz[t]))
        z_yz = [most(z_yz)]
    for i, worst in enumerate((dev_y, dev_z, y_yz, z_yz)):
        far_ref[i] = most(worst)


def wanted(plan_ref, mask_ref):
    plan = plan_ref[...]
    place = lax.broadcasted_iota(jnp.int32, plan.shape, 1)
    a, b, c = (
        jnp.sum(jnp.where(place == i, plan, 0), axis=1, keepdims=True)
        for i in range(3)
    )
    for i in range(mask_ref.shape[0]):
        asked = (i == a) | (i == 3 + 3 * a + b) | (i == 12 + c)
        mask_ref[i] = jnp.broadcast_to(
            jnp.where(asked, 1.0, 0.0), mask_ref.shape[1:]
        )


def folded(mask_ref, choices):
    worst = most(
        [jnp.where(mask_ref[i] > 0.0, v, 0.0) for i, v in choices.items()]
    )
    worst = jnp.max(worst, axis=0, keepdims=True)
    return jnp.maximum(worst, pltpu.roll(worst, COLS // 2, 1))


def together(
    own_ref, other_ref, high_ref, low_ref, mz_high_ref, mz_low_ref, my_ref,
    myz_ref, far_ref, mask_ref, share_ref,
):
    mx, mxz, dev_x, z_xz = [], [], [], []
    for y in range(4):
        mx.append(
            [
                (a + b) * 0.125
                for a, b in zip(tiles_of(own_ref, y), tiles_of(other_ref, y))
            ]
        )
        mxz.append(halves(mx[y]))
        for t in range(2 * SIDE):
            dev_x.append(
                both_ways(tile(high_ref, y, t), tile(low_ref, y, t), mx[y][t])
            )
        for t in range(SIDE):
            z_xz.append(
                both_ways(
                    tile(mz_high_ref, y, t), tile(mz_low_ref, y, t), mxz[y][t]
                )
            )
        dev_x, z_xz = [most(dev_x)], [most(z_xz)]
    mxy = over_gy(
        [
            functools.reduce(jnp.add, [mx[y][t] for y in range(4)])
            for t in range(2 * SIDE)
        ]
    )
    mall = halves(mxy)
    once = (*range(ONE), *range(SIDE, SIDE + ONE))
    x_xy = most([most(gaps(mx[y], mxy)) for y in range(4)])
    x_xz = most([most(gaps(mx[y][:SIDE], mxz[y])) for y in range(4)])
    y_xy = most(
        [jnp.abs(tile(my_ref, z, t) - mxy[t]) for z in range(4) for t in once]
    )
    xy_all = most(gaps(mxy[:ONE], mall))
    xz_all = most([most(gaps(mxz[y], mall)) for y in range(4)])
    yz_all = most(
        [
            jnp.abs(tile(myz_ref, z, t) - mall[t])
            for z in range(4)
            for t in range(ONE)
        ]
    )
    dev_y, dev_z, y_yz, z_yz = (far_ref[i] for i in range(4))
    first = folded(mask_ref, {0: dev_x[0], 1: dev_y, 2: dev_z})
    second = folded(
        mask_ref,
        {4: x_xy, 5: x_xz, 6: y_xy, 8: y_yz, 9: z_xz[0], 10: z_yz},
    )
    third = folded(mask_ref, {12: yz_all, 13: xz_all, 14: xy_all})
    lane = lax.broadcasted_iota(jnp.int32, (1, COLS), 1)
    told = [jnp.where(lane < COLS // 2, first, second), third]
    mean = jnp.concatenate(mall[:ONE], axis=0)
    mine = jnp.where(
        lax.axis_index("core") == 0, mean[:CORE], mean[CORE : 2 * CORE]
    )
    share = jnp.concatenate([mine, *told], axis=0)
    for i in range(share_ref.shape[0]):
        share_ref[i] = share


def begin(half_ref, out_ref, side, sems):
    count = half_ref.shape[0]
    part = count // sems.shape[0]
    copies = [
        pltpu.make_async_copy(
            half_ref.at[pl.ds(i * part, part), : CORE // 2],
            out_ref.at[pl.ds(i * part, part), side],
            sems.at[i],
        )
        for i in range(sems.shape[0])
    ]
    for copy in copies:
        copy.start()
    return copies


def put_own(own_ref, out_ref, worst_ref, sems):
    copies = begin(own_ref, out_ref, lax.axis_index("core"), sems)
    worst_ref[...] = jnp.max(own_ref[:, CORE // 2], axis=0)
    for copy in copies:
        copy.wait()


def put_other(
    worst_ref, other_ref, _, out_ref, reports_ref,
    reports_here, sems, reports_sem,
):
    copies = begin(other_ref, out_ref, 1 - lax.axis_index("core"), sems)
    worst = jnp.maximum(
        worst_ref[...], jnp.max(other_ref[:, CORE // 2], axis=0)
    )
    lane = lax.broadcasted_iota(jnp.int32, (1, COLS), 1)
    first = lane < COLS // 2
    reports_here[0] = jnp.max(jnp.where(first, worst[:1], 0.0))
    reports_here[1] = jnp.max(jnp.where(first, 0.0, worst[:1]))
    reports_here[2] = jnp.max(worst[1:])
    told = pltpu.make_async_copy(reports_here, reports_ref, reports_sem)
    told.start()
    for copy in (*copies, told):
        copy.wait()


def on_device(grads, plan):
    rows, width = grads.shape[-2:]
    tiles = width // COLS
    chips = lax.axis_size(PLANE)
    real = functools.partial(jax.ShapeDtypeStruct, dtype=jnp.float32)
    vmem = pl.BlockSpec(memory_space=pltpu.VMEM)
    hbm = pl.BlockSpec(memory_space=pl.ANY)
    kernel = functools.partial(pl.pallas_call, compiler_params=ROOM)
    under_swap = pl.CostEstimate(
        flops=10**7, bytes_accessed=grads.size * 4, transcendentals=0
    )
    cores = [(0, 1), (1, 0)]
    members = [
        [16 * z + 4 * y + x for z in YZ_ORDER for y in YZ_ORDER for x in X_ORDER]
    ]

    entries = grads.reshape(rows // 8, 8, tiles, COLS).transpose(0, 2, 1, 3)
    entries = entries.reshape(chips, CHIP // 2, 2, COLS)
    arrived = lax.all_to_all(
        entries, PLANE, 0, 0, tiled=True, axis_index_groups=members
    ).reshape(chips // 4, 4 * CHIP, COLS)
    four, side = real((4, 4 * CHIP, COLS)), real((4, 2 * CHIP, COLS))
    own_sum = kernel(sums, out_shape=four, in_specs=[vmem], out_specs=vmem)(
        arrived
    )
    other_sum = lax.ppermute(own_sum, "core", cores)
    local = kernel(
        alone,
        out_shape=(
            *(four, four, side, side, four, side),
            real((4, 8, COLS)),
        ),
        in_specs=[vmem],
        out_specs=(vmem,) * 7,
        cost_estimate=under_swap,
    )(arrived)
    mask = kernel(
        wanted,
        out_shape=real((15, 8, COLS)),
        in_specs=[vmem],
        out_specs=vmem,
        cost_estimate=under_swap,
    )(plan.reshape(1, -1))
    share = kernel(
        together,
        out_shape=real((chips, CARRIED, COLS)),
        in_specs=[vmem] * 10,
        out_specs=vmem,
    )(own_sum, other_sum, *local, mask)
    own = lax.all_to_all(
        share, PLANE, 0, 0, tiled=True, axis_index_groups=members
    ).reshape(chips, CARRIED // 2, 2, COLS)
    other = lax.ppermute(own, "core", cores)
    whole = real((chips, 2, CORE // 2, 2, COLS))
    begun, worst = kernel(
        put_own,
        out_shape=(whole, real((2, COLS))),
        in_specs=[vmem],
        out_specs=(hbm, vmem),
        scratch_shapes=[pltpu.SemaphoreType.DMA((2,))],
        cost_estimate=under_swap,
    )(own)
    whole, reports = kernel(
        put_other,
        out_shape=(whole, real((3,))),
        in_specs=[vmem, vmem, hbm],
        out_specs=(hbm, hbm),
        scratch_shapes=[
            pltpu.SMEM((3,), jnp.float32),
            pltpu.SemaphoreType.DMA((2,)),
            pltpu.SemaphoreType.DMA,
        ],
        input_output_aliases={2: 0},
    )(worst, other, begun)
    whole = whole.reshape(rows // 8, tiles, 8, COLS).transpose(0, 2, 1, 3)
    return whole.reshape(grads.shape), reports


def solution(mesh):
    torus = Mesh(
        mesh.devices.reshape(4, 2, 4, 2, mesh.shape["gz"]),
        ("z", "core", "y", "x_lo", "x_hi"),
    )
    placed = P(("z", "core"), ("y", "x_lo"), "x_hi", None, None)
    return jax.shard_map(
        on_device,
        mesh=torus,
        in_specs=(placed, P()),
        out_specs=(placed, P()),
        check_vma=False,
    )
```

```python
import functools

import jax
import jax.numpy as jnp
from jax import lax
from jax.experimental import pallas as pl
from jax.experimental.pallas import tpu as pltpu
from jax.sharding import Mesh
from jax.sharding import PartitionSpec as P

PLANE = ("y", "z", "x_hi", "x_lo")
YZ_ORDER, X_ORDER = (2, 0, 1, 3), (2, 3, 0, 1)
COLS = 128
CHIP = 28
CORE = CHIP // 2
CARRIED = 16
SIDE = 2 * CHIP // 8
ONE = 4
ROOM = pltpu.CompilerParams(vmem_limit_bytes=8 * 2**20)


def both_ways(high, low, mean):
    return jnp.maximum(high - mean, mean - low)


def most(values):
    return functools.reduce(jnp.maximum, values)


def gaps(tiles, means):
    return [jnp.abs(t - m) for t, m in zip(tiles, means)]


def stats(values):
    return (
        functools.reduce(jnp.add, values),
        functools.reduce(jnp.maximum, values),
        functools.reduce(jnp.minimum, values),
    )


def halves(tiles):
    return [(a + b) * 0.5 for a, b in zip(tiles[:SIDE], tiles[SIDE:])]


def across_x_lo(tiles):
    turned = [pltpu.roll(t, 4, 0) for t in tiles]
    first = lax.broadcasted_iota(jnp.int32, (8, COLS), 0) < 4
    return [
        jnp.where(first, turned[(t + 3) % SIDE], turned[(t + 4) % SIDE])
        for t in range(SIDE)
    ]


def over_gy(tiles):
    other = across_x_lo(tiles[:SIDE]) + across_x_lo(tiles[SIDE:])
    return [(a + b) * 0.125 for a, b in zip(tiles, other)]


def tile(ref, i, t):
    return ref[i, 8 * t : 8 * t + 8]


def tiles_of(ref, i):
    return [tile(ref, i, t) for t in range(ref.shape[1] // 8)]


def put(ref, i, tiles):
    for t, value in enumerate(tiles):
        ref[i, 8 * t : 8 * t + 8] = value


def sums(g_ref, sum_ref):
    for y in range(4):
        put(
            sum_ref,
            y,
            [
                functools.reduce(
                    jnp.add, [tile(g_ref, 4 * y + z, t) for z in range(4)]
                )
                for t in range(2 * SIDE)
            ],
        )


def alone(
    g_ref, high_ref, low_ref, mz_high_ref, mz_low_ref, my_ref, myz_ref, far_ref
):
    dev_z, z_yz = [], []
    mz_of_z = [[] for _ in range(4)]
    for y in range(4):
        high, low, mz_high, mz_low = [], [], [], []
        for t in range(SIDE):
            mz = []
            for half in (t, t + SIDE):
                values = [tile(g_ref, 4 * y + z, half) for z in range(4)]
                _, top, bottom = stats(values)
                high.append(top)
                low.append(bottom)
            for z in range(4):
                a = tile(g_ref, 4 * y + z, t)
                mean = (a + tile(g_ref, 4 * y + z, t + SIDE)) * 0.5
                dev_z.append(jnp.abs(a - mean))
                mz.append(mean)
            _, top, bottom = stats(mz)
            mz_high.append(top)
            mz_low.append(bottom)
            dev_z = [most(dev_z)]
        put(high_ref, y, high[::2] + high[1::2])
        put(low_ref, y, low[::2] + low[1::2])
        put(mz_high_ref, y, mz_high)
        put(mz_low_ref, y, mz_low)

    dev_y, y_yz = [], []
    for z in range(4):
        found = [
            stats([tile(g_ref, 4 * y + z, t) for y in range(4)])
            for t in range(2 * SIDE)
        ]
        my = over_gy([f[0] for f in found])
        myz = halves(my)
        put(my_ref, z, my)
        put(myz_ref, z, myz)
        dev_y.append(most([both_ways(f[1], f[2], m) for f, m in zip(found, my)]))
        y_yz.append(most(gaps(my[:ONE], myz)))
        for t in range(SIDE):
            mz = [
                (tile(g_ref, 4 * y + z, t) + tile(g_ref, 4 * y + z, t + SIDE))
                * 0.5
                for y in range(4)
            ]
            _, top, bottom = stats(mz)
            z_yz.append(both_ways(top, bottom, myz[t]))
        z_yz = [most(z_yz)]
    for i, worst in enumerate((dev_y, dev_z, y_yz, z_yz)):
        far_ref[i] = most(worst)


def wanted(plan_ref, mask_ref):
    plan = plan_ref[...]
    place = lax.broadcasted_iota(jnp.int32, plan.shape, 1)
    a, b, c = (
        jnp.sum(jnp.where(place == i, plan, 0), axis=1, keepdims=True)
        for i in range(3)
    )
    for i in range(mask_ref.shape[0]):
        asked = (i == a) | (i == 3 + 3 * a + b) | (i == 12 + c)
        mask_ref[i] = jnp.broadcast_to(
            jnp.where(asked, 1.0, 0.0), mask_ref.shape[1:]
        )


def folded(mask_ref, choices):
    worst = most(
        [jnp.where(mask_ref[i] > 0.0, v, 0.0) for i, v in choices.items()]
    )
    worst = jnp.max(worst, axis=0, keepdims=True)
    return jnp.maximum(worst, pltpu.roll(worst, COLS // 2, 1))


def together(
    own_ref, other_ref, high_ref, low_ref, mz_high_ref, mz_low_ref, my_ref,
    myz_ref, far_ref, mask_ref, share_ref,
):
    mx, mxz, dev_x, z_xz = [], [], [], []
    for y in range(4):
        mx.append(
            [
                (a + b) * 0.125
                for a, b in zip(tiles_of(own_ref, y), tiles_of(other_ref, y))
            ]
        )
        mxz.append(halves(mx[y]))
        for t in range(2 * SIDE):
            dev_x.append(
                both_ways(tile(high_ref, y, t), tile(low_ref, y, t), mx[y][t])
            )
        for t in range(SIDE):
            z_xz.append(
                both_ways(
                    tile(mz_high_ref, y, t), tile(mz_low_ref, y, t), mxz[y][t]
                )
            )
        dev_x, z_xz = [most(dev_x)], [most(z_xz)]
    mxy = over_gy(
        [
            functools.reduce(jnp.add, [mx[y][t] for y in range(4)])
            for t in range(2 * SIDE)
        ]
    )
    mall = halves(mxy)
    once = (*range(ONE), *range(SIDE, SIDE + ONE))
    x_xy = most([most(gaps(mx[y], mxy)) for y in range(4)])
    x_xz = most([most(gaps(mx[y][:SIDE], mxz[y])) for y in range(4)])
    y_xy = most(
        [jnp.abs(tile(my_ref, z, t) - mxy[t]) for z in range(4) for t in once]
    )
    xy_all = most(gaps(mxy[:ONE], mall))
    xz_all = most([most(gaps(mxz[y], mall)) for y in range(4)])
    yz_all = most(
        [
            jnp.abs(tile(myz_ref, z, t) - mall[t])
            for z in range(4)
            for t in range(ONE)
        ]
    )
    dev_y, dev_z, y_yz, z_yz = (far_ref[i] for i in range(4))
    first = folded(mask_ref, {0: dev_x[0], 1: dev_y, 2: dev_z})
    second = folded(
        mask_ref,
        {4: x_xy, 5: x_xz, 6: y_xy, 8: y_yz, 9: z_xz[0], 10: z_yz},
    )
    third = folded(mask_ref, {12: yz_all, 13: xz_all, 14: xy_all})
    lane = lax.broadcasted_iota(jnp.int32, (1, COLS), 1)
    told = [jnp.where(lane < COLS // 2, first, second), third]
    mean = jnp.concatenate(mall[:ONE], axis=0)
    mine = jnp.where(
        lax.axis_index("core") == 0, mean[:CORE], mean[CORE : 2 * CORE]
    )
    share = jnp.concatenate([mine, *told], axis=0)
    for i in range(share_ref.shape[0]):
        share_ref[i] = share


def begin(half_ref, out_ref, side, sems):
    count = half_ref.shape[0]
    part = count // sems.shape[0]
    copies = [
        pltpu.make_async_copy(
            half_ref.at[pl.ds(i * part, part), : CORE // 2],
            out_ref.at[pl.ds(i * part, part), side],
            sems.at[i],
        )
        for i in range(sems.shape[0])
    ]
    for copy in copies:
        copy.start()
    return copies


def put_own(own_ref, out_ref, worst_ref, sems):
    copies = begin(own_ref, out_ref, lax.axis_index("core"), sems)
    worst_ref[...] = jnp.max(own_ref[:, CORE // 2], axis=0)
    for copy in copies:
        copy.wait()


def put_other(
    worst_ref, other_ref, _, out_ref, reports_ref,
    reports_here, sems, reports_sem,
):
    copies = begin(other_ref, out_ref, 1 - lax.axis_index("core"), sems)
    worst = jnp.maximum(
        worst_ref[...], jnp.max(other_ref[:, CORE // 2], axis=0)
    )
    lane = lax.broadcasted_iota(jnp.int32, (1, COLS), 1)
    first = lane < COLS // 2
    reports_here[0] = jnp.max(jnp.where(first, worst[:1], 0.0))
    reports_here[1] = jnp.max(jnp.where(first, 0.0, worst[:1]))
    reports_here[2] = jnp.max(worst[1:])
    told = pltpu.make_async_copy(reports_here, reports_ref, reports_sem)
    told.start()
    for copy in (*copies, told):
        copy.wait()


def on_device(grads, plan):
    rows, width = grads.shape[-2:]
    tiles = width // COLS
    chips = lax.axis_size(PLANE)
    real = functools.partial(jax.ShapeDtypeStruct, dtype=jnp.float32)
    vmem = pl.BlockSpec(memory_space=pltpu.VMEM)
    hbm = pl.BlockSpec(memory_space=pl.ANY)
    kernel = functools.partial(pl.pallas_call, compiler_params=ROOM)
    under_swap = pl.CostEstimate(
        flops=10**7, bytes_accessed=grads.size * 4, transcendentals=0
    )
    cores = [(0, 1), (1, 0)]
    members = [
        [16 * y + 4 * z + x for y in YZ_ORDER for z in YZ_ORDER for x in X_ORDER]
    ]

    entries = grads.reshape(rows // 8, 8, tiles, COLS).transpose(0, 2, 1, 3)
    entries = entries.reshape(chips, CHIP // 2, 2, COLS)
    arrived = lax.all_to_all(
        entries, PLANE, 0, 0, tiled=True, axis_index_groups=members
    ).reshape(chips // 4, 4 * CHIP, COLS)
    four, side = real((4, 4 * CHIP, COLS)), real((4, 2 * CHIP, COLS))
    own_sum = kernel(sums, out_shape=four, in_specs=[vmem], out_specs=vmem)(
        arrived
    )
    other_sum = lax.ppermute(own_sum, "core", cores)
    local = kernel(
        alone,
        out_shape=(
            *(four, four, side, side, four, side),
            real((4, 8, COLS)),
        ),
        in_specs=[vmem],
        out_specs=(vmem,) * 7,
        cost_estimate=under_swap,
    )(arrived)
    mask = kernel(
        wanted,
        out_shape=real((15, 8, COLS)),
        in_specs=[vmem],
        out_specs=vmem,
        cost_estimate=under_swap,
    )(plan.reshape(1, -1))
    share = kernel(
        together,
        out_shape=real((chips, CARRIED, COLS)),
        in_specs=[vmem] * 10,
        out_specs=vmem,
    )(own_sum, other_sum, *local, mask)
    own = lax.all_to_all(
        share, PLANE, 0, 0, tiled=True, axis_index_groups=members
    ).reshape(chips, CARRIED // 2, 2, COLS)
    other = lax.ppermute(own, "core", cores)
    whole = real((chips, 2, CORE // 2, 2, COLS))
    begun, worst = kernel(
        put_own,
        out_shape=(whole, real((2, COLS))),
        in_specs=[vmem],
        out_specs=(hbm, vmem),
        scratch_shapes=[pltpu.SemaphoreType.DMA((1,))],
        cost_estimate=under_swap,
    )(own)
    whole, reports = kernel(
        put_other,
        out_shape=(whole, real((3,))),
        in_specs=[vmem, vmem, hbm],
        out_specs=(hbm, hbm),
        scratch_shapes=[
            pltpu.SMEM((3,), jnp.float32),
            pltpu.SemaphoreType.DMA((1,)),
            pltpu.SemaphoreType.DMA,
        ],
        input_output_aliases={2: 0},
    )(worst, other, begun)
    whole = whole.reshape(rows // 8, tiles, 8, COLS).transpose(0, 2, 1, 3)
    return whole.reshape(grads.shape), reports


def solution(mesh):
    torus = Mesh(
        mesh.devices.reshape(4, 2, 4, 2, mesh.shape["gz"]),
        ("z", "core", "y", "x_lo", "x_hi"),
    )
    placed = P(("z", "core"), ("y", "x_lo"), "x_hi", None, None)
    return jax.shard_map(
        on_device,
        mesh=torus,
        in_specs=(placed, P()),
        out_specs=(placed, P()),
        check_vma=False,
    )
```
